256 devices in a mesh: dp: 32 (over y, z), rows: 8 (over x, core).
Axes of the slice: x: 4, y: 4, z: 8, core: 2. Of those that a mesh axis runs over, the one named last changes fastest.
Arguments:
- item_ids: int32 [32768], P(('dp', 'rows')), may hold values from 0 to 4095, as said below
- lengths: int32 [256, 4], P(('dp', 'rows')), may hold values from 1 to 64, 128 in all within a row
- item_table: bfloat16 [4096, 512], P('rows'), may hold values from -6 to 6
- in_weight: bfloat16 [512, 2048], replicated, may hold values from -0.25 to 0.25
- out_weight: bfloat16 [512, 512], replicated, may hold values from -0.25 to 0.25
- grad_out: bfloat16 [32768, 512], P(('dp', 'rows')), may hold values from -6 to 6
Outputs:
- mixed_rows: bfloat16 [32768, 512], P(('dp', 'rows'))
- table_grad: float32 [4096, 512], P('rows')
The draws below stay inside these ranges and needn't reach their ends.
Inputs may be any that keep to these rules, and one draw needn't show every extreme that they name: `item_ids`: table shard s holds items s*512 to (s+1)*512 - 1. The 128 IDs of each block fall at most 32 times into any one shard, and exactly 32 times into one shard of every block. `lengths`: each row sums to 128, and its largest entry is exactly 64.
All inputs are finite; a program needn't handle non-finite values.
Results may differ from the reference program's by a relative error of at most 0.0064.
Values may be sent and summed in bfloat16 or wider, within the bound.
A program may use at most 64 MiB of HBM per device.

```python
import math
import jax
import jax.numpy as jnp
import numpy as np
from jax import lax

D = 512
HEADS = 8
TOK_DEV = 128
USERS = 4
V_SHARD = 512
MAXLEN = 64
CAP = 32
VOCAB = 4096
TOKENS = 32768
N_DP = 32
N_ROWS = 8


def shuffle_tokens(subkey):
    return jax.random.permutation(subkey, TOK_DEV)


def shuffle_owners(subkey):
    return jax.random.permutation(subkey, N_ROWS)


def draw_item_ids(key, part):
    blocks = TOKENS // TOK_DEV
    base = jax.random.fold_in(key, 17)
    key_ranking, key_holder, key_offset = jax.random.split(base, 3)
    ranking = jax.vmap(shuffle_tokens)(jax.random.split(key_ranking, blocks))
    remaining = TOK_DEV - CAP
    shares = [CAP] + [remaining * (index + 1) // (N_ROWS - 1) - remaining * index // (N_ROWS - 1) for index in range(N_ROWS - 1)]
    bounds = jnp.asarray(np.cumsum(np.array(shares, dtype=np.int64))[:-1], dtype=jnp.int32)
    slot_rank = jnp.sum((ranking[:, :, None] >= bounds[None, None, :]).astype(jnp.int32), axis=2)
    holders = jax.vmap(shuffle_owners)(jax.random.split(key_holder, blocks))
    holder = jnp.take_along_axis(holders, slot_rank, axis=1)
    offset = jax.random.randint(key_offset, (blocks, TOK_DEV), 0, V_SHARD)
    return (holder * V_SHARD + offset).reshape(TOKENS).astype(jnp.int32)


def level_of(stream_key, shape, cuts, low, largest):
    factor_of = 1.0
    for axis_at, blocks in cuts:
        heights = jax.random.uniform(jax.random.fold_in(jax.random.fold_in(stream_key, 6), axis_at), (blocks,), jnp.float32, low / len(cuts), largest / len(cuts))
        factor_of = factor_of * jnp.repeat(jnp.exp(heights), shape[axis_at] // blocks).reshape((-1,) + (1,) * (len(shape) - 1 - axis_at))
    return factor_of


def profile(count, total, bound, slope):
    loads = [(1 << 20) // math.isqrt(grade ** slope) + 1 for grade in range(2, count + 1)]
    rest, given = total - bound - (count - 1), [1] * (count - 1)
    while rest > 0:
        candidates = [i for i in range(count - 1) if given[i] < bound]
        mass, left = sum([loads[i] for i in candidates]), rest
        for i in candidates:
            extra = min(bound - given[i], max(1, left * loads[i] // mass), rest)
            given[i] = given[i] + extra
            rest = rest - extra
    return np.array([bound] + given)


def ragged_sizes(stream_key, amount, total, most, skew):
    if amount == 2:
        one = jax.random.randint(stream_key, (), max(1, total - most), min(most, total - 1) + 1)
        return jnp.stack([one, total - one])
    sizes = jnp.asarray(profile(amount, total, most, skew), jnp.int32)
    twos = (amount - 1) // 2
    donor, receiver = sizes[1:1 + 2 * twos:2], sizes[2:2 + 2 * twos:2]
    room = jnp.minimum(donor - 1, most - receiver)
    shifted = jax.random.randint(jax.random.fold_in(stream_key, 1), (twos,), 0, 1 << 20) % (room + 1)
    sizes = sizes.at[1:1 + 2 * twos:2].set(donor - shifted).at[2:2 + 2 * twos:2].set(receiver + shifted)
    return sizes[jax.random.permutation(jax.random.fold_in(stream_key, 2), amount)]


def centred(stream_key, dims, width, reach, shards=(), held_as=jnp.bfloat16):
    result = jax.random.normal(stream_key, dims, jnp.float32) * width
    if len(shards) > 0:
        result = level_of(stream_key, dims, shards, -0.22, 0.18) * result
    return jnp.clip(result, min=-reach, max=reach).astype(held_as)


def setup_inputs(seed: int = 0) -> dict:
    key_list = jax.random.split(jax.random.key(seed), 7)
    item_ids = draw_item_ids(jax.random.fold_in(key_list[6], 71), 0)
    lengths = jax.vmap(lambda own: ragged_sizes(own, USERS, TOK_DEV, MAXLEN, 2))(jax.random.split(key_list[1], (N_DP * N_ROWS))).reshape((N_DP * N_ROWS, USERS)).astype(jnp.int32)
    item_table = centred(key_list[2], (VOCAB, D), 1.0, 6.0, ((0, 8),))
    in_weight = centred(key_list[3], (D, 4 * D), D ** -0.5, 0.25)
    out_weight = centred(key_list[4], (D, D), D ** -0.5, 0.25)
    grad_out = centred(key_list[5], (TOKENS, D), 1.0, 6.0, ((0, 256),))
    return {"item_ids": item_ids, "lengths": lengths, "item_table": item_table, "in_weight": in_weight, "out_weight": out_weight, "grad_out": grad_out}


EPS = 1e-06

def contract_last(left, right):
    return lax.dot_general(left, right, (((1,), (1,)), ((), ())), preferred_element_type=jnp.float32)

def batched(form, left, right):
    return jnp.einsum(form, left.astype(jnp.float32), right.astype(jnp.float32))

def hstu_layer(rows, lengths_row, cotangent, in_weight, out_weight):
    tokens, features = rows.shape
    head_count = HEADS
    head_size = features // head_count
    score_scale = head_size ** (-0.5)
    input_wide = rows.astype(jnp.float32)
    row_scale = lax.rsqrt(lax.optimization_barrier(jnp.mean(input_wide * input_wide, axis=-1, keepdims=True)) + EPS)
    unit_input = input_wide * row_scale
    normed = unit_input.astype(jnp.bfloat16)
    projected = jnp.dot(normed, in_weight, preferred_element_type=jnp.float32)
    sigmoid_proj = jax.nn.sigmoid(projected)
    activated = projected * sigmoid_proj
    gate_units = activated[:, :features]
    value_heads = activated[:, features:2 * features].astype(jnp.bfloat16).reshape(tokens, head_count, head_size)
    query_heads = activated[:, 2 * features:3 * features].astype(jnp.bfloat16).reshape(tokens, head_count, head_size)
    key_heads = activated[:, 3 * features:].astype(jnp.bfloat16).reshape(tokens, head_count, head_size)
    places = jnp.arange(tokens, dtype=jnp.int32)
    user_ends = jnp.cumsum(lengths_row).astype(jnp.int32)
    user_of = lax.optimization_barrier(jnp.sum((places[:, None] >= user_ends[None, :]).astype(jnp.int32), axis=1))
    allowed = ((user_of[:, None] == user_of[None, :]) & (places[None, :] <= places[:, None])).astype(jnp.float32)
    scores = batched('qhd,khd->hqk', query_heads, key_heads) * score_scale
    sigmoid_score = jax.nn.sigmoid(scores)
    weights = (scores * sigmoid_score * allowed / MAXLEN).astype(jnp.bfloat16)
    attended = batched('hqk,khd->qhd', weights, value_heads).reshape(tokens, features)
    attended_scale = lax.rsqrt(lax.optimization_barrier(jnp.mean(attended * attended, axis=-1, keepdims=True)) + EPS)
    unit_output = attended * attended_scale
    gated_out = (unit_output * gate_units).astype(jnp.bfloat16)
    layer_out = (input_wide + jnp.dot(gated_out, out_weight, preferred_element_type=jnp.float32)).astype(jnp.bfloat16)
    grad_gated = contract_last(cotangent, out_weight)
    grad_gate = grad_gated * unit_output
    grad_unit = grad_gated * gate_units
    grad_att = attended_scale * (grad_unit - unit_output * lax.optimization_barrier(jnp.mean(grad_unit * unit_output, axis=-1, keepdims=True)))
    grad_att = grad_att.astype(jnp.bfloat16).reshape(tokens, head_count, head_size)
    grad_weights = batched('qhd,khd->hqk', grad_att, value_heads)
    grad_values = batched('hqk,qhd->khd', weights, grad_att).reshape(tokens, features)
    grad_scores = grad_weights * allowed / MAXLEN * sigmoid_score * (1.0 + scores * (1.0 - sigmoid_score)) * score_scale
    grad_scores = grad_scores.astype(jnp.bfloat16)
    grad_queries = batched('hqk,khd->qhd', grad_scores, key_heads).reshape(tokens, features)
    grad_keys = batched('hqk,qhd->khd', grad_scores, query_heads).reshape(tokens, features)
    grad_activated = jnp.concatenate([grad_gate, grad_values, grad_queries, grad_keys], axis=1)
    grad_pre = (grad_activated * sigmoid_proj * (1.0 + projected * (1.0 - sigmoid_proj))).astype(jnp.bfloat16)
    grad_normed = contract_last(grad_pre, in_weight)
    grad_rows = cotangent.astype(jnp.float32) + row_scale * (grad_normed - unit_input * lax.optimization_barrier(jnp.mean(grad_normed * unit_input, axis=-1, keepdims=True)))
    return (layer_out, grad_rows)

def reference(item_ids, lengths, item_table, in_weight, out_weight, grad_out):
    blocks = TOKENS // TOK_DEV
    looked_up = jnp.take(item_table, item_ids, axis=0).reshape(blocks, TOK_DEV, D)
    cotangents = grad_out.reshape(blocks, TOK_DEV, D)

    def one_block(inputs):
        return hstu_layer(inputs[0], inputs[1], inputs[2], in_weight, out_weight)
    outputs = lax.map(one_block, (looked_up, lengths, cotangents))
    grad_rows = outputs[1].reshape(TOKENS, D)
    table_grad = jax.ops.segment_sum(grad_rows, item_ids, num_segments=VOCAB)
    return (outputs[0].reshape(TOKENS, D), table_grad)
```

```python
import functools

import jax
import jax.numpy as jnp
from jax import lax
from jax.experimental import pallas as pl
from jax.experimental.pallas import tpu as pltpu
from jax.sharding import PartitionSpec as P

HEADS = 8
MAXLEN = 64
EPS = 1e-06
NY = 4
CHUNKS = 2
F32 = jnp.float32
BF16 = jnp.bfloat16
I32 = jnp.int32
ROW_ORDER = (4, 3, 5, 2, 6, 1, 7)
Y_ORDER = (2, 1, 3)
Z_ORDER = (4, 3, 5, 2, 6, 1, 7)


def mm(left, right):
    return jnp.dot(left, right, preferred_element_type=F32)


def mm_last(left, right):
    return lax.dot_general(left, right, (((1,), (1,)), ((), ())), preferred_element_type=F32)


def mm_first(left, right):
    return lax.dot_general(left, right, (((0,), (0,)), ((), ())), preferred_element_type=F32)


def iota(shape, dim):
    return lax.broadcasted_iota(I32, shape, dim)


def kernel(
    owners,
    nz,
    ids_hbm,
    lens_hbm,
    table_hbm,
    win_hbm,
    wout_hbm,
    cot_hbm,
    out_ref,
    tg_ref,
    ids_v,
    ids_all,
    lens_s,
    tab,
    win,
    wout,
    cot_v,
    rsend,
    fetched,
    at_s,
    pt_s,
    p_s,
    gg_s,
    allow_s,
    dact_s,
    gate_s,
    vqk_s,
    w_s,
    dsw_s,
    att_s,
    gpre_s,
    gsend,
    grecv,
    ysend,
    yrecv,
    zsend,
    zrecv,
    local_sem,
    ids_ss,
    ids_rs,
    row_ss,
    row_rs,
    x_ss,
    x_rs,
    y_ss,
    y_rs,
    z_ss,
    z_rs,
    az_ss,
    az_rs,
    ay_ss,
    ay_rs,
):
    tokens = ids_v.shape[1]
    shard_rows, features = tab.shape
    cap = rsend.shape[1]
    me = lax.axis_index("rows")
    dp = lax.axis_index("dp")
    yi = dp // nz
    zi = lax.rem(dp, nz)

    def row_dev(k):
        return (dp, lax.rem(me + owners - k, owners))

    def y_of(k):
        return lax.rem(yi + k, NY)

    def z_of(k):
        return lax.rem(zi + k, nz)

    def y_dev(k):
        return (y_of(k) * nz + zi, me)

    def z_dev(k):
        return (yi * nz + z_of(k), me)

    def rcopy(src, dst, ss, rs, dev):
        return pltpu.make_async_remote_copy(
            src_ref=src,
            dst_ref=dst,
            send_sem=ss,
            recv_sem=rs,
            device_id=dev,
            device_id_type=pl.DeviceIdType.MESH,
        )

    ids_load = pltpu.make_async_copy(ids_hbm, ids_v, local_sem.at[0])
    lens_load = pltpu.make_async_copy(lens_hbm, lens_s, local_sem.at[1])
    tab_load = pltpu.make_async_copy(table_hbm, tab, local_sem.at[2])
    win_load = pltpu.make_async_copy(win_hbm, win, local_sem.at[3])
    wout_load = pltpu.make_async_copy(wout_hbm, wout, local_sem.at[4])
    cot_load = pltpu.make_async_copy(cot_hbm, cot_v, local_sem.at[5])
    ids_load.start()
    lens_load.start()

    barrier = pltpu.get_barrier_semaphore()
    peers = 0
    for k in Z_ORDER:
        pl.semaphore_signal(barrier, inc=1, device_id=z_dev(k), device_id_type=pl.DeviceIdType.MESH)
        peers += 1
    for k in Y_ORDER:
        pl.semaphore_signal(barrier, inc=1, device_id=y_dev(k), device_id_type=pl.DeviceIdType.MESH)
        peers += 1
    for k in ROW_ORDER:
        pl.semaphore_signal(
            barrier, inc=1, device_id=row_dev(k), device_id_type=pl.DeviceIdType.MESH
        )
        peers += 1
    tab_load.start()
    cot_load.start()
    wout_load.start()
    win_load.start()
    ids_load.wait()
    pl.semaphore_wait(barrier, peers)

    ids_copies = []
    for k in ROW_ORDER:
        back = owners - k
        c = rcopy(ids_v, ids_all.at[back], ids_ss.at[back], ids_rs.at[back], row_dev(k))
        c.start()
        ids_copies.append(c)

    ids = ids_v[...]
    before = (iota((tokens, tokens), 0) < iota((tokens, tokens), 1)).astype(BF16)
    rel = lax.rem(me + owners - ids // shard_rows, owners)
    memb = rel == iota((owners, tokens), 0)
    rank = mm(memb.astype(BF16), before)
    slot_row = jnp.sum(
        jnp.where(memb, rank + (iota((owners, tokens), 0) * cap).astype(F32), 0.0),
        axis=0,
        keepdims=True,
    )
    slot_ids = iota((owners * cap, tokens), 0).astype(F32)
    pt_s[...] = (slot_ids == slot_row).astype(BF16)
    diag = iota((tokens, tokens), 0) == iota((tokens, tokens), 1)
    slot_col = jnp.sum(
        jnp.where(diag, jnp.broadcast_to(slot_row, (tokens, tokens)), 0.0), axis=1, keepdims=True
    )
    p_s[...] = (iota((tokens, owners * cap), 1).astype(F32) == slot_col).astype(BF16)

    lens_load.wait()
    ends = []
    total = lens_s[0, 0]
    ends.append(total)
    for u in range(1, lens_s.shape[1]):
        total = total + lens_s[0, u]
        ends.append(total)
    ti = iota((tokens, tokens), 0)
    tj = iota((tokens, tokens), 1)
    ui = sum((ti >= e).astype(I32) for e in ends)
    uj = sum((tj >= e).astype(I32) for e in ends)
    allow_s[...] = jnp.where((ui == uj) & (tj <= ti), 1.0 / MAXLEN, 0.0)

    for c in ids_copies:
        c.wait_recv()
    lo = me * shard_rows
    ids_mat = jnp.concatenate([ids] + [ids_all[k] for k in range(1, owners)], axis=0)
    mine = (ids_mat >= lo) & (ids_mat < lo + shard_rows)
    mrank = mm(mine.astype(BF16), before)
    key = jnp.where(mine, mrank, -1.0)
    off1 = jnp.where(mine, (ids_mat - lo + 1).astype(F32), 0.0)
    slots = iota((cap, tokens), 0).astype(F32)
    cols = []
    for k in range(owners):
        cols.append(
            jnp.sum(
                jnp.where(slots == key[k : k + 1, :], off1[k : k + 1, :], 0.0),
                axis=1,
                keepdims=True,
            )
        )
    off_col = jnp.concatenate(cols, axis=0) - 1.0
    pick = (iota((owners * cap, shard_rows), 1).astype(F32) == off_col).astype(BF16)
    tab_load.wait()
    found = mm(pick, tab[...]).astype(BF16)
    rsend[...] = found.reshape(owners, cap, features)
    row_copies = []
    for k in ROW_ORDER:
        c = rcopy(
            rsend.at[k], fetched.at[owners - k], row_ss.at[owners - k], row_rs.at[owners - k], row_dev(k)
        )
        c.start()
        row_copies.append(c)
    fetched[0] = rsend[0]

    at_s[...] = pick.T
    cot_load.wait()
    wout_load.wait()
    gg_s[...] = mm_last(cot_v[...], wout[...])
    win_load.wait()

    for c in row_copies:
        c.wait_recv()
    x = mm(p_s[...], fetched[...].reshape(owners * cap, features))
    row_scale = lax.rsqrt(jnp.mean(x * x, axis=-1, keepdims=True) + EPS)
    unit_x = x * row_scale
    normed = unit_x.astype(BF16)
    width = 256
    for j in range(4 * features // width):
        here = slice(j * width, (j + 1) * width)
        p = mm(normed, win[:, here])
        s = jax.nn.sigmoid(p)
        a = p * s
        dact_s[:, here] = s * (1.0 + p * (1.0 - s))
        if j * width < features:
            gate_s[:, here] = a
        else:
            vqk_s[:, j * width - features : (j + 1) * width - features] = a.astype(BF16)

    pair = 2 * (features // HEADS)
    low = iota((tokens, pair), 1) < pair // 2
    allow = allow_s[...]
    allow2 = jnp.concatenate([allow, allow], axis=0)
    zero = jnp.zeros((tokens, pair), BF16)

    def split(b):
        return jnp.concatenate([jnp.where(low, b, zero), jnp.where(low, zero, b)], axis=0)

    def beside(b):
        return jnp.concatenate([b[:tokens], b[tokens:]], axis=1)

    score_scale = (features // HEADS) ** (-0.5)
    for g in range(HEADS // 2):
        v2 = vqk_s[:, g * pair : (g + 1) * pair]
        q2 = vqk_s[:, features + g * pair : features + (g + 1) * pair]
        k2 = vqk_s[:, 2 * features + g * pair : 2 * features + (g + 1) * pair]
        s = mm_last(split(q2), k2) * score_scale
        sg = jax.nn.sigmoid(s)
        w = (s * sg * allow2).astype(BF16)
        w_s[g] = w
        dsw_s[g] = allow2 * sg * (1.0 + s * (1.0 - sg)) * score_scale
        att_s[:, g * pair : (g + 1) * pair] = mm(beside(w), split(v2))

    att = att_s[...]
    att_scale = lax.rsqrt(jnp.mean(att * att, axis=-1, keepdims=True) + EPS)
    unit_o = att * att_scale
    gate = gate_s[...]
    gg = gg_s[...]
    grad_unit = gg * gate
    ga = att_scale * (grad_unit - unit_o * jnp.mean(grad_unit * unit_o, axis=-1, keepdims=True))
    ga = ga.astype(BF16)
    gpre_s[:, :features] = (gg * unit_o * dact_s[:, :features]).astype(BF16)
    gated = (unit_o * gate).astype(BF16)
    for g in range(HEADS // 2):
        v_at = slice(features + g * pair, features + (g + 1) * pair)
        q_at = slice(2 * features + g * pair, 2 * features + (g + 1) * pair)
        k_at = slice(3 * features + g * pair, 3 * features + (g + 1) * pair)
        v2 = vqk_s[:, g * pair : (g + 1) * pair]
        q2 = vqk_s[:, features + g * pair : features + (g + 1) * pair]
        k2 = vqk_s[:, 2 * features + g * pair : 2 * features + (g + 1) * pair]
        gas = split(ga[:, g * pair : (g + 1) * pair])
        gw = mm_last(gas, v2)
        ds = (gw * dsw_s[g]).astype(BF16)
        gv = mm_first(w_s[g], gas)
        gq = mm(beside(ds), split(k2))
        gk = mm_first(ds, split(q2))
        gpre_s[:, v_at] = (gv * dact_s[:, v_at]).astype(BF16)
        gpre_s[:, q_at] = (gq * dact_s[:, q_at]).astype(BF16)
        gpre_s[:, k_at] = (gk * dact_s[:, k_at]).astype(BF16)
    gn = mm_last(gpre_s[...], win[...])
    grad_rows = cot_v[...].astype(F32) + row_scale * (
        gn - unit_x * jnp.mean(gn * unit_x, axis=-1, keepdims=True)
    )
    outgoing = mm(pt_s[...], grad_rows.astype(BF16)).astype(BF16)
    gsend[...] = outgoing.reshape(owners, cap, features)
    cw = features // CHUNKS
    x_copies, y_copies, z_copies, az_copies, ay_copies = [], [], [], [], []
    for c in range(CHUNKS):
        at = pl.ds(c * cw, cw)
        for k in ROW_ORDER:
            d = rcopy(
                gsend.at[k, :, at],
                grecv.at[owners - k, :, at],
                x_ss.at[c, owners - k],
                x_rs.at[c, owners - k],
                row_dev(k),
            )
            d.start()
            x_copies.append(d)
    grecv[0] = gsend[0]

    out_ref[...] = (x + mm(gated, wout[...])).astype(BF16)

    peer_count = owners - 1
    for c in range(CHUNKS):
        here = slice(c * cw, (c + 1) * cw)
        at = pl.ds(c * cw, cw)
        for d in x_copies[c * peer_count : (c + 1) * peer_count]:
            d.wait_recv()
        dense = mm(at_s[...], grecv[:, :, here].reshape(owners * cap, cw)).astype(BF16)
        ysend[:, :, here] = dense.reshape(NY, shard_rows // NY, cw)
        for k in Y_ORDER:
            d = rcopy(
                ysend.at[y_of(k), :, at], yrecv.at[k, :, at], y_ss.at[c, k], y_rs.at[c, k], y_dev(k)
            )
            d.start()
            y_copies.append(d)
    for c in range(CHUNKS):
        here = slice(c * cw, (c + 1) * cw)
        at = pl.ds(c * cw, cw)
        for d in y_copies[c * (NY - 1) : (c + 1) * (NY - 1)]:
            d.wait_recv()
        part = ysend[yi, :, here].astype(F32)
        for k in range(1, NY):
            part = part + yrecv[k, :, here].astype(F32)
        zsend[:, :, here] = part.astype(BF16).reshape(nz, shard_rows // (NY * nz), cw)
        for k in Z_ORDER:
            d = rcopy(
                zsend.at[z_of(k), :, at], zrecv.at[k, :, at], z_ss.at[c, k], z_rs.at[c, k], z_dev(k)
            )
            d.start()
            z_copies.append(d)
    for c in range(CHUNKS):
        here = slice(c * cw, (c + 1) * cw)
        at = pl.ds(c * cw, cw)
        for d in z_copies[c * (nz - 1) : (c + 1) * (nz - 1)]:
            d.wait_recv()
        part = zsend[zi, :, here].astype(F32)
        for k in range(1, nz):
            part = part + zrecv[k, :, here].astype(F32)
        tg_ref[yi, zi, :, here] = part.astype(BF16)
        for k in Z_ORDER:
            d = rcopy(
                tg_ref.at[yi, zi, :, at],
                tg_ref.at[yi, zi, :, at],
                az_ss.at[c, k],
                az_rs.at[c, k],
                z_dev(k),
            )
            d.start()
            az_copies.append(d)
    for c in range(CHUNKS):
        at = pl.ds(c * cw, cw)
        for k in Z_ORDER:
            came = lax.rem(zi + nz - k, nz)
            rcopy(
                tg_ref.at[yi, came, :, at],
                tg_ref.at[yi, came, :, at],
                az_ss.at[c, k],
                az_rs.at[c, k],
                z_dev(k),
            ).wait_recv()
        for k in Y_ORDER:
            d = rcopy(
                tg_ref.at[yi, :, :, at],
                tg_ref.at[yi, :, :, at],
                ay_ss.at[c, k],
                ay_rs.at[c, k],
                y_dev(k),
            )
            d.start()
            ay_copies.append(d)
    for c in range(CHUNKS):
        at = pl.ds(c * cw, cw)
        for k in Y_ORDER:
            came = lax.rem(yi + NY - k, NY)
            rcopy(
                tg_ref.at[came, :, :, at],
                tg_ref.at[came, :, :, at],
                ay_ss.at[c, k],
                ay_rs.at[c, k],
                y_dev(k),
            ).wait_recv()
    for d in ids_copies + row_copies + x_copies + y_copies + z_copies + az_copies + ay_copies:
        d.wait_send()


def solution(mesh):
    owners = mesh.shape["rows"]
    nz = mesh.shape["dp"] // NY

    def shards(item_ids, lengths, item_table, in_weight, out_weight, grad_out):
        tokens = item_ids.shape[0]
        shard_rows, features = item_table.shape
        cap = 2 * tokens // owners
        piece = shard_rows // (NY * nz)
        dma = pltpu.SemaphoreType.DMA
        any_spec = pl.BlockSpec(memory_space=pl.ANY)
        vmem = pl.BlockSpec(memory_space=pltpu.VMEM)
        heads2 = HEADS // 2
        mixed, table_grad = pl.pallas_call(
            functools.partial(kernel, owners, nz),
            name="hstu",
            out_shape=(
                jax.ShapeDtypeStruct((tokens, features), BF16),
                jax.ShapeDtypeStruct((NY, nz, piece, features), BF16),
            ),
            in_specs=[any_spec] * 6,
            out_specs=(vmem, vmem),
            scratch_shapes=[
                pltpu.VMEM((1, tokens), I32),
                pltpu.VMEM((owners, 1, tokens), I32),
                pltpu.SMEM(lengths.shape, I32),
                pltpu.VMEM((shard_rows, features), BF16),
                pltpu.VMEM(in_weight.shape, BF16),
                pltpu.VMEM(out_weight.shape, BF16),
                pltpu.VMEM((tokens, features), BF16),
                pltpu.VMEM((owners, cap, features), BF16),
                pltpu.VMEM((owners, cap, features), BF16),
                pltpu.VMEM((shard_rows, owners * cap), BF16),
                pltpu.VMEM((owners * cap, tokens), BF16),
                pltpu.VMEM((tokens, owners * cap), BF16),
                pltpu.VMEM((tokens, features), F32),
                pltpu.VMEM((tokens, tokens), F32),
                pltpu.VMEM((tokens, 4 * features), F32),
                pltpu.VMEM((tokens, features), F32),
                pltpu.VMEM((tokens, 3 * features), BF16),
                pltpu.VMEM((heads2, 2 * tokens, tokens), BF16),
                pltpu.VMEM((heads2, 2 * tokens, tokens), F32),
                pltpu.VMEM((tokens, features), F32),
                pltpu.VMEM((tokens, 4 * features), BF16),
                pltpu.VMEM((owners, cap, features), BF16),
                pltpu.VMEM((owners, cap, features), BF16),
                pltpu.VMEM((NY, shard_rows // NY, features), BF16),
                pltpu.VMEM((NY, shard_rows // NY, features), BF16),
                pltpu.VMEM((nz, piece, features), BF16),
                pltpu.VMEM((nz, piece, features), BF16),
                dma((6,)),
                dma((owners,)),
                dma((owners,)),
                dma((owners,)),
                dma((owners,)),
                dma((CHUNKS, owners)),
                dma((CHUNKS, owners)),
                dma((CHUNKS, NY)),
                dma((CHUNKS, NY)),
                dma((CHUNKS, nz)),
                dma((CHUNKS, nz)),
                dma((CHUNKS, nz)),
                dma((CHUNKS, nz)),
                dma((CHUNKS, NY)),
                dma((CHUNKS, NY)),
            ],
            compiler_params=pltpu.CompilerParams(
                collective_id=0, has_side_effects=True, vmem_limit_bytes=40 * 1024 * 1024
            ),
        )(
            item_ids.reshape(1, tokens),
            lengths,
            item_table,
            in_weight,
            out_weight,
            grad_out,
        )
        return mixed, table_grad.reshape(shard_rows, features).astype(F32)

    return jax.shard_map(
        shards,
        mesh=mesh,
        in_specs=(
            P(("dp", "rows")),
            P(("dp", "rows"), None),
            P("rows", None),
            P(),
            P(),
            P(("dp", "rows"), None),
        ),
        out_specs=(P(("dp", "rows"), None), P("rows", None)),
        check_vma=False,
    )
```

```python
import functools

import jax
import jax.numpy as jnp
from jax import lax
from jax.experimental import pallas as pl
from jax.experimental.pallas import tpu as pltpu
from jax.sharding import PartitionSpec as P

HEADS = 8
MAXLEN = 64
EPS = 1e-06
NY = 4
CHUNKS = 2
DELIVERIES = 4
F32 = jnp.float32
BF16 = jnp.bfloat16
I32 = jnp.int32
ROW_ORDER = (4, 3, 5, 2, 6, 1, 7)
Y_ORDER = (2, 1, 3)
Z_ORDER = (4, 3, 5, 2, 6, 1, 7, 0)
Z_RUNS = ((0, 3), (3, 5), (5, 7), (7, 8))
MESH = pl.DeviceIdType.MESH


def mm(left, right):
    return jnp.dot(left, right, preferred_element_type=F32)


def mm_last(left, right):
    return lax.dot_general(left, right, (((1,), (1,)), ((), ())), preferred_element_type=F32)


def mm_first(left, right):
    return lax.dot_general(left, right, (((0,), (0,)), ((), ())), preferred_element_type=F32)


def iota(shape, dim):
    return lax.broadcasted_iota(I32, shape, dim)


def kernel(
    owners,
    nz,
    ids_hbm,
    lens_hbm,
    table_hbm,
    win_hbm,
    wout_hbm,
    cot_hbm,
    out_ref,
    tg_ref,
    ids_v,
    ids_all,
    lens_s,
    tab,
    win,
    wout,
    cot_v,
    rsend,
    fetched,
    at_s,
    pt_s,
    p_s,
    gg_s,
    allow_s,
    dact_s,
    gate_s,
    vqk_s,
    w_s,
    dsw_s,
    att_s,
    gpre_s,
    gsend,
    grecv,
    ysend,
    yrecv,
    zsend,
    zrecv,
    own_s,
    local_sem,
    send_sem,
    in_sem,
    x_rs,
    y_rs,
    z_rs,
    az_rs,
    near_sem,
    far_sem,
):
    tokens = ids_v.shape[1]
    shard_rows, features = tab.shape
    cap = rsend.shape[1]
    piece = zsend.shape[1]
    cw = features // CHUNKS
    me = lax.axis_index("rows")
    dp = lax.axis_index("dp")
    yi = dp // nz
    zi = lax.rem(dp, nz)

    def row_dev(k):
        return (dp, lax.rem(me + owners - k, owners))

    def y_of(k):
        return lax.rem(yi + k, NY)

    def z_of(k):
        return lax.rem(zi + k, nz)

    def y_dev(k):
        return (y_of(k) * nz + zi, me)

    def z_dev(k):
        return (yi * nz + z_of(k), me)

    def rcopy(src, dst, ss, rs, dev):
        return pltpu.make_async_remote_copy(
            src_ref=src, dst_ref=dst, send_sem=ss, recv_sem=rs, device_id=dev, device_id_type=MESH
        )

    def signal(sem, dev):
        pl.semaphore_signal(sem, inc=1, device_id=dev, device_id_type=MESH)

    s_ids, s_row, s_x, s_y, s_z, s_az, s_ay = (send_sem.at[i] for i in range(7))
    in_ids, in_row, in_ay = (in_sem.at[i] for i in range(3))

    def came(ref, sem):
        rcopy(ref, ref, s_ids, sem, row_dev(1)).wait_recv()

    def gone(ref, sem):
        rcopy(ref, ref, sem, in_ids, row_dev(1)).wait_send()

    ids_load = pltpu.make_async_copy(ids_hbm, ids_v, local_sem.at[0])
    lens_load = pltpu.make_async_copy(lens_hbm, lens_s, local_sem.at[1])
    tab_load = pltpu.make_async_copy(table_hbm, tab, local_sem.at[2])
    win_load = pltpu.make_async_copy(win_hbm, win, local_sem.at[3])
    wout_load = pltpu.make_async_copy(wout_hbm, wout, local_sem.at[4])
    cot_load = pltpu.make_async_copy(cot_hbm, cot_v, local_sem.at[5])
    ids_load.start()

    barrier = pltpu.get_barrier_semaphore()
    for k in ROW_ORDER:
        signal(barrier, row_dev(k))
    for k in (1, NY - 1):
        signal(barrier, y_dev(k))
    for k in (1, nz - 1):
        signal(barrier, z_dev(k))
    tab_load.start()
    lens_load.start()
    cot_load.start()
    wout_load.start()
    win_load.start()
    ids_load.wait()
    pl.semaphore_wait(barrier, len(ROW_ORDER) + 4)

    for k in ROW_ORDER:
        rcopy(ids_v, ids_all.at[owners - k], s_ids, in_ids, row_dev(k)).start()
    for k in (1, nz - 1):
        signal(near_sem, z_dev(k))
    for k in (1, NY - 1):
        signal(near_sem, y_dev(k))

    ids = ids_v[...]
    before = (iota((tokens, tokens), 0) < iota((tokens, tokens), 1)).astype(BF16)
    rel = lax.rem(me + owners - ids // shard_rows, owners)
    memb = rel == iota((owners, tokens), 0)
    rank = mm(memb.astype(BF16), before)
    slot_row = jnp.sum(
        jnp.where(memb, rank + (iota((owners, tokens), 0) * cap).astype(F32), 0.0),
        axis=0,
        keepdims=True,
    )
    slot_ids = iota((owners * cap, tokens), 0).astype(F32)
    pt_s[...] = (slot_ids == slot_row).astype(BF16)
    diag = iota((tokens, tokens), 0) == iota((tokens, tokens), 1)
    slot_col = jnp.sum(
        jnp.where(diag, jnp.broadcast_to(slot_row, (tokens, tokens)), 0.0), axis=1, keepdims=True
    )
    p_s[...] = (iota((tokens, owners * cap), 1).astype(F32) == slot_col).astype(BF16)

    lens_load.wait()
    ends = []
    total = lens_s[0, 0]
    ends.append(total)
    for u in range(1, lens_s.shape[1]):
        total = total + lens_s[0, u]
        ends.append(total)
    ti = iota((tokens, tokens), 0)
    tj = iota((tokens, tokens), 1)
    ui = sum((ti >= e).astype(I32) for e in ends)
    uj = sum((tj >= e).astype(I32) for e in ends)
    allow_s[...] = jnp.where((ui == uj) & (tj <= ti), 1.0 / MAXLEN, 0.0)

    came(ids_all.at[pl.ds(1, owners - 1)], in_ids)
    lo = me * shard_rows
    ids_mat = jnp.concatenate([ids] + [ids_all[k] for k in range(1, owners)], axis=0)
    mine = (ids_mat >= lo) & (ids_mat < lo + shard_rows)
    mrank = mm(mine.astype(BF16), before)
    key = jnp.where(mine, mrank, -1.0)
    off1 = jnp.where(mine, (ids_mat - lo + 1).astype(F32), 0.0)
    slots = iota((cap, tokens), 0).astype(F32)
    cols = []
    for k in range(owners):
        cols.append(
            jnp.sum(
                jnp.where(slots == key[k : k + 1, :], off1[k : k + 1, :], 0.0),
                axis=1,
                keepdims=True,
            )
        )
    off_col = jnp.concatenate(cols, axis=0) - 1.0
    pick = (iota((owners * cap, shard_rows), 1).astype(F32) == off_col).astype(BF16)
    tab_load.wait()
    found = mm(pick, tab[...]).astype(BF16)
    rsend[...] = found.reshape(owners, cap, features)
    for k in ROW_ORDER:
        rcopy(rsend.at[k], fetched.at[owners - k], s_row, in_row, row_dev(k)).start()
    fetched[0] = rsend[0]

    spot = iota((1, shard_rows), 1)
    run_at = lax.rem(spot // piece, nz)
    along_z = sum(jnp.where(run_at == i, z, 0) for i, z in enumerate(Z_ORDER))
    item = (
        lax.rem(yi + spot // (piece * nz), NY) * (piece * nz)
        + lax.rem(zi + along_z, nz) * piece
        + lax.rem(spot, piece)
    )
    at_s[...] = (item.astype(F32) == off_col).astype(BF16).T
    cot_load.wait()
    wout_load.wait()
    gg_s[...] = mm_last(cot_v[...], wout[...])
    win_load.wait()
    pl.semaphore_wait(near_sem, 4)
    for k in (2, nz - 2):
        signal(far_sem, z_dev(k))

    came(fetched.at[pl.ds(1, owners - 1)], in_row)
    x = mm(p_s[...], fetched[...].reshape(owners * cap, features))
    row_scale = lax.rsqrt(jnp.mean(x * x, axis=-1, keepdims=True) + EPS)
    unit_x = x * row_scale
    normed = unit_x.astype(BF16)
    width = 256
    for j in range(4 * features // width):
        here = slice(j * width, (j + 1) * width)
        p = mm(normed, win[:, here])
        s = jax.nn.sigmoid(p)
        a = p * s
        dact_s[:, here] = s * (1.0 + p * (1.0 - s))
        if j * width < features:
            gate_s[:, here] = a
        else:
            vqk_s[:, j * width - features : (j + 1) * width - features] = a.astype(BF16)

    pair = 2 * (features // HEADS)
    low = iota((tokens, pair), 1) < pair // 2
    allow = allow_s[...]
    allow2 = jnp.concatenate([allow, allow], axis=0)
    zero = jnp.zeros((tokens, pair), BF16)

    def split(b):
        return jnp.concatenate([jnp.where(low, b, zero), jnp.where(low, zero, b)], axis=0)

    def beside(b):
        return jnp.concatenate([b[:tokens], b[tokens:]], axis=1)

    score_scale = (features // HEADS) ** (-0.5)
    for g in range(HEADS // 2):
        v2 = vqk_s[:, g * pair : (g + 1) * pair]
        q2 = vqk_s[:, features + g * pair : features + (g + 1) * pair]
        k2 = vqk_s[:, 2 * features + g * pair : 2 * features + (g + 1) * pair]
        s = mm_last(split(q2), k2) * score_scale
        sg = jax.nn.sigmoid(s)
        w = (s * sg * allow2).astype(BF16)
        w_s[g] = w
        dsw_s[g] = allow2 * sg * (1.0 + s * (1.0 - sg)) * score_scale
        att_s[:, g * pair : (g + 1) * pair] = mm(beside(w), split(v2))

    att = att_s[...]
    att_scale = lax.rsqrt(jnp.mean(att * att, axis=-1, keepdims=True) + EPS)
    unit_o = att * att_scale
    gate = gate_s[...]
    gg = gg_s[...]
    grad_unit = gg * gate
    ga = att_scale * (grad_unit - unit_o * jnp.mean(grad_unit * unit_o, axis=-1, keepdims=True))
    ga = ga.astype(BF16)
    gpre_s[:, :features] = (gg * unit_o * dact_s[:, :features]).astype(BF16)
    gated = (unit_o * gate).astype(BF16)
    for g in range(HEADS // 2):
        v_at = slice(features + g * pair, features + (g + 1) * pair)
        q_at = slice(2 * features + g * pair, 2 * features + (g + 1) * pair)
        k_at = slice(3 * features + g * pair, 3 * features + (g + 1) * pair)
        v2 = vqk_s[:, g * pair : (g + 1) * pair]
        q2 = vqk_s[:, features + g * pair : features + (g + 1) * pair]
        k2 = vqk_s[:, 2 * features + g * pair : 2 * features + (g + 1) * pair]
        gas = split(ga[:, g * pair : (g + 1) * pair])
        gw = mm_last(gas, v2)
        ds = (gw * dsw_s[g]).astype(BF16)
        gv = mm_first(w_s[g], gas)
        gq = mm(beside(ds), split(k2))
        gk = mm_first(ds, split(q2))
        gpre_s[:, v_at] = (gv * dact_s[:, v_at]).astype(BF16)
        gpre_s[:, q_at] = (gq * dact_s[:, q_at]).astype(BF16)
        gpre_s[:, k_at] = (gk * dact_s[:, k_at]).astype(BF16)
    gn = mm_last(gpre_s[...], win[...])
    grad_rows = cot_v[...].astype(F32) + row_scale * (
        gn - unit_x * jnp.mean(gn * unit_x, axis=-1, keepdims=True)
    )
    outgoing = mm(pt_s[...], grad_rows.astype(BF16)).astype(BF16)
    gsend[...] = outgoing.reshape(owners, cap, features)
    for c in range(CHUNKS):
        at = pl.ds(c * cw, cw)
        for k in ROW_ORDER:
            rcopy(gsend.at[k, :, at], grecv.at[owners - k, :, at], s_x, x_rs.at[c], row_dev(k)).start()
    grecv[0] = gsend[0]

    out_ref[...] = (x + mm(gated, wout[...])).astype(BF16)
    pl.semaphore_wait(far_sem, 2)

    for c in range(CHUNKS):
        here = slice(c * cw, (c + 1) * cw)
        at = pl.ds(c * cw, cw)
        came(grecv.at[pl.ds(1, owners - 1), :, at], x_rs.at[c])
        dense = mm(at_s[...], grecv[:, :, here].reshape(owners * cap, cw)).astype(BF16)
        ysend[:, :, :, here] = dense.reshape(NY, nz, piece, cw)
        for r, (p0, p1) in enumerate(Z_RUNS):
            run = pl.ds(p0, p1 - p0)
            for k in Y_ORDER:
                rcopy(
                    ysend.at[k, run, :, at],
                    yrecv.at[k, run, :, at],
                    s_y,
                    y_rs.at[c * len(Z_RUNS) + r],
                    y_dev(k),
                ).start()
    for c in range(CHUNKS):
        here = slice(c * cw, (c + 1) * cw)
        at = pl.ds(c * cw, cw)
        for r, (p0, p1) in enumerate(Z_RUNS):
            run = pl.ds(p0, p1 - p0)
            came(yrecv.at[pl.ds(1, NY - 1), run, :, at], y_rs.at[c * len(Z_RUNS) + r])
            part = ysend[0, p0:p1, :, here].astype(F32)
            for k in range(1, NY):
                part = part + yrecv[k, p0:p1, :, here].astype(F32)
            if Z_ORDER[p0] == 0:
                own_s[:, here] = part[0]
                continue
            zsend[p0:p1, :, here] = part.astype(BF16)
            for p in range(p0, p1):
                rcopy(
                    zsend.at[p, :, at], zrecv.at[p, :, at], s_z, z_rs.at[c], z_dev(Z_ORDER[p])
                ).start()

    def along_y(c, z):
        ref = tg_ref.at[yi, z, :, pl.ds(c * cw, cw)]
        for k in Y_ORDER:
            rcopy(ref, ref, s_ay, in_ay, y_dev(k)).start()

    for c in range(CHUNKS):
        here = slice(c * cw, (c + 1) * cw)
        at = pl.ds(c * cw, cw)
        came(zrecv.at[pl.ds(0, nz - 1), :, at], z_rs.at[c])
        part = own_s[:, here]
        for p in range(nz - 1):
            part = part + zrecv[p, :, here].astype(F32)
        tg_ref[yi, zi, :, here] = part.astype(BF16)
        ref = tg_ref.at[yi, zi, :, at]
        for r, (p0, p1) in enumerate(Z_RUNS[:-1]):
            for p in range(p0, p1):
                rcopy(ref, ref, s_az, az_rs.at[c * 3 + r], z_dev(Z_ORDER[p])).start()
        along_y(c, zi)
    for c in range(CHUNKS):
        at = pl.ds(c * cw, cw)
        for r in (2, 1, 0):
            p0, p1 = Z_RUNS[r]
            came(zrecv.at[pl.ds(p0, p1 - p0), :, at], az_rs.at[c * 3 + r])
            for p in range(p0, p1):
                along_y(c, lax.rem(zi + nz - Z_ORDER[p], nz))
    came(tg_ref.at[pl.ds(0, NY - 1)], in_ay)
    gone(ids_all.at[pl.ds(1, owners - 1)], s_ids)
    gone(rsend.at[pl.ds(1, owners - 1)], s_row)
    gone(gsend.at[pl.ds(1, owners - 1)], s_x)
    gone(ysend.at[pl.ds(1, NY - 1)], s_y)
    gone(zsend.at[pl.ds(0, nz - 1)], s_z)
    gone(zsend.at[pl.ds(0, nz - 1)], s_az)
    gone(tg_ref.at[pl.ds(0, NY - 1)], s_ay)


def deliver(mixed_ref, tg_ref, out_hbm, grad_hbm, wide, sem):
    first = pltpu.make_async_copy(mixed_ref, out_hbm, sem.at[0])
    first.start()
    rows = wide.shape[0] // DELIVERIES
    copies = []
    for i in range(DELIVERIES):
        at = slice(i * rows, (i + 1) * rows)
        wide[at, :] = tg_ref[at, :].astype(F32)
        c = pltpu.make_async_copy(
            wide.at[pl.ds(i * rows, rows)], grad_hbm.at[pl.ds(i * rows, rows)], sem.at[i + 1]
        )
        c.start()
        copies.append(c)
    first.wait()
    for c in copies:
        c.wait()


def solution(mesh):
    owners = mesh.shape["rows"]
    nz = mesh.shape["dp"] // NY

    def shards(item_ids, lengths, item_table, in_weight, out_weight, grad_out):
        tokens = item_ids.shape[0]
        shard_rows, features = item_table.shape
        cap = 2 * tokens // owners
        piece = shard_rows // (NY * nz)
        dma = pltpu.SemaphoreType.DMA
        any_spec = pl.BlockSpec(memory_space=pl.ANY)
        vmem = pl.BlockSpec(memory_space=pltpu.VMEM)
        heads2 = HEADS // 2
        mixed, table_grad = pl.pallas_call(
            functools.partial(kernel, owners, nz),
            name="hstu",
            out_shape=(
                jax.ShapeDtypeStruct((tokens, features), BF16),
                jax.ShapeDtypeStruct((NY, nz, piece, features), BF16),
            ),
            in_specs=[any_spec] * 6,
            out_specs=(vmem, vmem),
            scratch_shapes=[
                pltpu.VMEM((1, tokens), I32),
                pltpu.VMEM((owners, 1, tokens), I32),
                pltpu.SMEM(lengths.shape, I32),
                pltpu.VMEM((shard_rows, features), BF16),
                pltpu.VMEM(in_weight.shape, BF16),
                pltpu.VMEM(out_weight.shape, BF16),
                pltpu.VMEM((tokens, features), BF16),
                pltpu.VMEM((owners, cap, features), BF16),
                pltpu.VMEM((owners, cap, features), BF16),
                pltpu.VMEM((shard_rows, owners * cap), BF16),
                pltpu.VMEM((owners * cap, tokens), BF16),
                pltpu.VMEM((tokens, owners * cap), BF16),
                pltpu.VMEM((tokens, features), F32),
                pltpu.VMEM((tokens, tokens), F32),
                pltpu.VMEM((tokens, 4 * features), F32),
                pltpu.VMEM((tokens, features), F32),
                pltpu.VMEM((tokens, 3 * features), BF16),
                pltpu.VMEM((heads2, 2 * tokens, tokens), BF16),
                pltpu.VMEM((heads2, 2 * tokens, tokens), F32),
                pltpu.VMEM((tokens, features), F32),
                pltpu.VMEM((tokens, 4 * features), BF16),
                pltpu.VMEM((owners, cap, features), BF16),
                pltpu.VMEM((owners, cap, features), BF16),
                pltpu.VMEM((NY, nz, piece, features), BF16),
                pltpu.VMEM((NY, nz, piece, features), BF16),
                pltpu.VMEM((nz, piece, features), BF16),
                pltpu.VMEM((nz, piece, features), BF16),
                pltpu.VMEM((piece, features), F32),
                dma((6,)),
                dma((7,)),
                dma((3,)),
                dma((CHUNKS,)),
                dma((CHUNKS * len(Z_RUNS),)),
                dma((CHUNKS,)),
                dma((CHUNKS * 3,)),
                pltpu.SemaphoreType.REGULAR,
                pltpu.SemaphoreType.REGULAR,
            ],
            compiler_params=pltpu.CompilerParams(
                collective_id=0, has_side_effects=True, vmem_limit_bytes=40 * 1024 * 1024
            ),
        )(
            *[
                pltpu.with_memory_space_constraint(v, pltpu.HBM)
                for v in (item_ids.reshape(1, tokens), lengths, item_table, in_weight, out_weight, grad_out)
            ]
        )
        return pl.pallas_call(
            deliver,
            name="deliver",
            out_shape=(
                jax.ShapeDtypeStruct((tokens, features), BF16),
                jax.ShapeDtypeStruct((shard_rows, features), F32),
            ),
            in_specs=[vmem, vmem],
            out_specs=(any_spec, any_spec),
            scratch_shapes=[pltpu.VMEM((shard_rows, features), F32), dma((DELIVERIES + 1,))],
            compiler_params=pltpu.CompilerParams(vmem_limit_bytes=8 * 1024 * 1024),
        )(mixed, table_grad.reshape(shard_rows, features))

    return jax.shard_map(
        shards,
        mesh=mesh,
        in_specs=(
            P(("dp", "rows")),
            P(("dp", "rows"), None),
            P("rows", None),
            P(),
            P(),
            P(("dp", "rows"), None),
        ),
        out_specs=(P(("dp", "rows"), None), P("rows", None)),
        check_vma=False,
    )
```

```python
import functools

import jax
import jax.numpy as jnp
from jax import lax
from jax.experimental import pallas as pl
from jax.experimental.pallas import tpu as pltpu
from jax.sharding import PartitionSpec as P

HEADS = 8
MAXLEN = 64
EPS = 1e-06
NY = 4
CHUNKS = 2
DELIVERIES = 4
F32 = jnp.float32
BF16 = jnp.bfloat16
I32 = jnp.int32
ROW_ORDER = (4, 3, 5, 2, 6, 1, 7)
Y_ORDER = (2, 1, 3)
Z_ORDER = (4, 3, 5, 2, 6, 1, 7, 0)
Z_FAR, Z_OWN = 0, 7
Z_RUNS = ((1, 3), (3, 5), (5, 7))
MESH = pl.DeviceIdType.MESH


def mm(left, right):
    return jnp.dot(left, right, preferred_element_type=F32)


def mm_last(left, right):
    return lax.dot_general(left, right, (((1,), (1,)), ((), ())), preferred_element_type=F32)


def mm_first(left, right):
    return lax.dot_general(left, right, (((0,), (0,)), ((), ())), preferred_element_type=F32)


def iota(shape, dim):
    return lax.broadcasted_iota(I32, shape, dim)


def kernel(
    owners,
    nz,
    ids_hbm,
    lens_hbm,
    table_hbm,
    win_hbm,
    wout_hbm,
    cot_hbm,
    out_ref,
    tg_ref,
    ids_v,
    ids_all,
    lens_s,
    tab,
    win,
    wout,
    cot_v,
    rsend,
    fetched,
    at_s,
    pt_s,
    p_s,
    gg_s,
    allow_s,
    dact_s,
    gate_s,
    vqk_s,
    w_s,
    dsw_s,
    att_s,
    gpre_s,
    gsend,
    grecv,
    ysend,
    yrecv,
    zsend,
    zrecv,
    own_s,
    far_in,
    own_send,
    local_sem,
    send_sem,
    in_sem,
    x_rs,
    y_rs,
    z_rs,
    az_rs,
    far_rs,
    yo_rs,
    near_sem,
    far_sem,
):
    tokens = ids_v.shape[1]
    shard_rows, features = tab.shape
    cap = rsend.shape[1]
    piece = zsend.shape[1]
    cw = features // CHUNKS
    me = lax.axis_index("rows")
    dp = lax.axis_index("dp")
    yi = dp // nz
    zi = lax.rem(dp, nz)

    def row_dev(k):
        return (dp, lax.rem(me + owners - k, owners))

    def y_of(k):
        return lax.rem(yi + k, NY)

    def z_of(k):
        return lax.rem(zi + k, nz)

    def y_dev(k):
        return (y_of(k) * nz + zi, me)

    def z_dev(k):
        return (yi * nz + z_of(k), me)

    def rcopy(src, dst, ss, rs, dev):
        return pltpu.make_async_remote_copy(
            src_ref=src, dst_ref=dst, send_sem=ss, recv_sem=rs, device_id=dev, device_id_type=MESH
        )

    def signal(sem, dev):
        pl.semaphore_signal(sem, inc=1, device_id=dev, device_id_type=MESH)

    s_ids, s_row, s_x, s_y, s_z, s_az, s_ay = (send_sem.at[i] for i in range(7))
    in_ids, in_row, in_ay = (in_sem.at[i] for i in range(3))

    def came(ref, sem):
        rcopy(ref, ref, s_ids, sem, row_dev(1)).wait_recv()

    def gone(ref, sem):
        rcopy(ref, ref, sem, in_ids, row_dev(1)).wait_send()

    ids_load = pltpu.make_async_copy(ids_hbm, ids_v, local_sem.at[0])
    lens_load = pltpu.make_async_copy(lens_hbm, lens_s, local_sem.at[1])
    tab_load = pltpu.make_async_copy(table_hbm, tab, local_sem.at[2])
    win_load = pltpu.make_async_copy(win_hbm, win, local_sem.at[3])
    wout_load = pltpu.make_async_copy(wout_hbm, wout, local_sem.at[4])
    cot_load = pltpu.make_async_copy(cot_hbm, cot_v, local_sem.at[5])
    ids_load.start()

    barrier = pltpu.get_barrier_semaphore()
    for k in ROW_ORDER:
        signal(barrier, row_dev(k))
    for k in (1, NY - 1):
        signal(barrier, y_dev(k))
    for k in (1, nz - 1):
        signal(barrier, z_dev(k))
    tab_load.start()
    lens_load.start()
    cot_load.start()
    wout_load.start()
    win_load.start()
    ids_load.wait()
    pl.semaphore_wait(barrier, len(ROW_ORDER) + 4)

    for k in ROW_ORDER:
        rcopy(ids_v, ids_all.at[owners - k], s_ids, in_ids, row_dev(k)).start()
    for k in (1, nz - 1):
        signal(near_sem, z_dev(k))
    for k in (1, NY - 1):
        signal(near_sem, y_dev(k))

    ids = ids_v[...]
    before = (iota((tokens, tokens), 0) < iota((tokens, tokens), 1)).astype(BF16)
    rel = lax.rem(me + owners - ids // shard_rows, owners)
    memb = rel == iota((owners, tokens), 0)
    rank = mm(memb.astype(BF16), before)
    slot_row = jnp.sum(
        jnp.where(memb, rank + (iota((owners, tokens), 0) * cap).astype(F32), 0.0),
        axis=0,
        keepdims=True,
    )
    slot_ids = iota((owners * cap, tokens), 0).astype(F32)
    pt_s[...] = (slot_ids == slot_row).astype(BF16)
    diag = iota((tokens, tokens), 0) == iota((tokens, tokens), 1)
    slot_col = jnp.sum(
        jnp.where(diag, jnp.broadcast_to(slot_row, (tokens, tokens)), 0.0), axis=1, keepdims=True
    )
    p_s[...] = (iota((tokens, owners * cap), 1).astype(F32) == slot_col).astype(BF16)

    lens_load.wait()
    ends = []
    total = lens_s[0, 0]
    ends.append(total)
    for u in range(1, lens_s.shape[1]):
        total = total + lens_s[0, u]
        ends.append(total)
    ti = iota((tokens, tokens), 0)
    tj = iota((tokens, tokens), 1)
    ui = sum((ti >= e).astype(I32) for e in ends)
    uj = sum((tj >= e).astype(I32) for e in ends)
    allow_s[...] = jnp.where((ui == uj) & (tj <= ti), 1.0 / MAXLEN, 0.0)

    came(ids_all.at[pl.ds(1, owners - 1)], in_ids)
    lo = me * shard_rows
    ids_mat = jnp.concatenate([ids] + [ids_all[k] for k in range(1, owners)], axis=0)
    mine = (ids_mat >= lo) & (ids_mat < lo + shard_rows)
    mrank = mm(mine.astype(BF16), before)
    key = jnp.where(mine, mrank, -1.0)
    off1 = jnp.where(mine, (ids_mat - lo + 1).astype(F32), 0.0)
    slots = iota((cap, tokens), 0).astype(F32)
    cols = []
    for k in range(owners):
        cols.append(
            jnp.sum(
                jnp.where(slots == key[k : k + 1, :], off1[k : k + 1, :], 0.0),
                axis=1,
                keepdims=True,
            )
        )
    off_col = jnp.concatenate(cols, axis=0) - 1.0
    pick = (iota((owners * cap, shard_rows), 1).astype(F32) == off_col).astype(BF16)
    tab_load.wait()
    found = mm(pick, tab[...]).astype(BF16)
    rsend[...] = found.reshape(owners, cap, features)
    for k in ROW_ORDER:
        rcopy(rsend.at[k], fetched.at[owners - k], s_row, in_row, row_dev(k)).start()
    fetched[0] = rsend[0]

    spot = iota((1, shard_rows), 1)
    run_at = lax.rem(spot // piece, nz)
    along_z = sum(jnp.where(run_at == i, z, 0) for i, z in enumerate(Z_ORDER))
    item = (
        lax.rem(yi + spot // (piece * nz), NY) * (piece * nz)
        + lax.rem(zi + along_z, nz) * piece
        + lax.rem(spot, piece)
    )
    at_s[...] = (item.astype(F32) == off_col).astype(BF16).T
    cot_load.wait()
    wout_load.wait()
    gg_s[...] = mm_last(cot_v[...], wout[...])
    win_load.wait()
    pl.semaphore_wait(near_sem, 4)
    for k in (2, nz - 2):
        signal(far_sem, z_dev(k))

    came(fetched.at[pl.ds(1, owners - 1)], in_row)
    x = mm(p_s[...], fetched[...].reshape(owners * cap, features))
    row_scale = lax.rsqrt(jnp.mean(x * x, axis=-1, keepdims=True) + EPS)
    unit_x = x * row_scale
    normed = unit_x.astype(BF16)
    width = 256
    for j in range(4 * features // width):
        here = slice(j * width, (j + 1) * width)
        p = mm(normed, win[:, here])
        s = jax.nn.sigmoid(p)
        a = p * s
        dact_s[:, here] = s * (1.0 + p * (1.0 - s))
        if j * width < features:
            gate_s[:, here] = a
        else:
            vqk_s[:, j * width - features : (j + 1) * width - features] = a.astype(BF16)

    pair = 2 * (features // HEADS)
    low = iota((tokens, pair), 1) < pair // 2
    allow = allow_s[...]
    allow2 = jnp.concatenate([allow, allow], axis=0)
    zero = jnp.zeros((tokens, pair), BF16)

    def split(b):
        return jnp.concatenate([jnp.where(low, b, zero), jnp.where(low, zero, b)], axis=0)

    def beside(b):
        return jnp.concatenate([b[:tokens], b[tokens:]], axis=1)

    score_scale = (features // HEADS) ** (-0.5)
    for g in range(HEADS // 2):
        v2 = vqk_s[:, g * pair : (g + 1) * pair]
        q2 = vqk_s[:, features + g * pair : features + (g + 1) * pair]
        k2 = vqk_s[:, 2 * features + g * pair : 2 * features + (g + 1) * pair]
        s = mm_last(split(q2), k2) * score_scale
        sg = jax.nn.sigmoid(s)
        w = (s * sg * allow2).astype(BF16)
        w_s[g] = w
        dsw_s[g] = allow2 * sg * (1.0 + s * (1.0 - sg)) * score_scale
        att_s[:, g * pair : (g + 1) * pair] = mm(beside(w), split(v2))

    att = att_s[...]
    att_scale = lax.rsqrt(jnp.mean(att * att, axis=-1, keepdims=True) + EPS)
    unit_o = att * att_scale
    gate = gate_s[...]
    gg = gg_s[...]
    grad_unit = gg * gate
    ga = att_scale * (grad_unit - unit_o * jnp.mean(grad_unit * unit_o, axis=-1, keepdims=True))
    ga = ga.astype(BF16)
    gpre_s[:, :features] = (gg * unit_o * dact_s[:, :features]).astype(BF16)
    gated = (unit_o * gate).astype(BF16)
    for g in range(HEADS // 2):
        v_at = slice(features + g * pair, features + (g + 1) * pair)
        q_at = slice(2 * features + g * pair, 2 * features + (g + 1) * pair)
        k_at = slice(3 * features + g * pair, 3 * features + (g + 1) * pair)
        v2 = vqk_s[:, g * pair : (g + 1) * pair]
        q2 = vqk_s[:, features + g * pair : features + (g + 1) * pair]
        k2 = vqk_s[:, 2 * features + g * pair : 2 * features + (g + 1) * pair]
        gas = split(ga[:, g * pair : (g + 1) * pair])
        gw = mm_last(gas, v2)
        ds = (gw * dsw_s[g]).astype(BF16)
        gv = mm_first(w_s[g], gas)
        gq = mm(beside(ds), split(k2))
        gk = mm_first(ds, split(q2))
        gpre_s[:, v_at] = (gv * dact_s[:, v_at]).astype(BF16)
        gpre_s[:, q_at] = (gq * dact_s[:, q_at]).astype(BF16)
        gpre_s[:, k_at] = (gk * dact_s[:, k_at]).astype(BF16)
    gn = mm_last(gpre_s[...], win[...])
    grad_rows = cot_v[...].astype(F32) + row_scale * (
        gn - unit_x * jnp.mean(gn * unit_x, axis=-1, keepdims=True)
    )
    outgoing = mm(pt_s[...], grad_rows.astype(BF16)).astype(BF16)
    gsend[...] = outgoing.reshape(owners, cap, features)
    for c in range(CHUNKS):
        at = pl.ds(c * cw, cw)
        for k in ROW_ORDER:
            rcopy(gsend.at[k, :, at], grecv.at[owners - k, :, at], s_x, x_rs.at[c], row_dev(k)).start()
    grecv[0] = gsend[0]

    out_ref[...] = (x + mm(gated, wout[...])).astype(BF16)
    pl.semaphore_wait(far_sem, 2)

    runs = len(Z_RUNS)

    def cut(c):
        return slice(c * cw, (c + 1) * cw), pl.ds(c * cw, cw)

    for c in range(CHUNKS):
        here, at = cut(c)
        came(grecv.at[pl.ds(1, owners - 1), :, at], x_rs.at[c])
        dense = mm(at_s[...], grecv[:, :, here].reshape(owners * cap, cw)).astype(BF16)
        ysend[:, :, :, here] = dense.reshape(NY, nz, piece, cw)
        rcopy(
            ysend.at[:, Z_FAR, :, at],
            far_in.at[:, :, at],
            s_z,
            far_rs.at[c],
            z_dev(Z_ORDER[Z_FAR]),
        ).start()
        for r, (p0, p1) in enumerate(Z_RUNS):
            run = pl.ds(p0, p1 - p0)
            for k in Y_ORDER:
                rcopy(
                    ysend.at[k, run, :, at],
                    yrecv.at[k, run, :, at],
                    s_y,
                    y_rs.at[c * runs + r],
                    y_dev(k),
                ).start()

    def over_y(c, r):
        here, at = cut(c)
        p0, p1 = Z_RUNS[r]
        came(yrecv.at[pl.ds(1, NY - 1), pl.ds(p0, p1 - p0), :, at], y_rs.at[c * runs + r])
        part = ysend[0, p0:p1, :, here].astype(F32)
        for k in range(1, NY):
            part = part + yrecv[k, p0:p1, :, here].astype(F32)
        zsend[p0:p1, :, here] = part.astype(BF16)
        for p in range(p0, p1):
            rcopy(
                zsend.at[p, :, at], zrecv.at[p, :, at], s_z, z_rs.at[c], z_dev(Z_ORDER[p])
            ).start()

    def over_far(c):
        here, at = cut(c)
        came(far_in.at[:, :, at], far_rs.at[c])
        part = ysend[:, Z_OWN, :, here].astype(F32) + far_in[:, :, here].astype(F32)
        own_s[:, here] = part[0]
        own_send[:, :, here] = part.astype(BF16)
        for k in Y_ORDER:
            rcopy(
                own_send.at[k, :, at], yrecv.at[k, Z_OWN, :, at], s_y, yo_rs.at[c], y_dev(k)
            ).start()

    def leave(c):
        here, at = cut(c)
        came(yrecv.at[pl.ds(1, NY - 1), Z_OWN, :, at], yo_rs.at[c])
        part = own_s[:, here]
        for k in range(1, NY):
            part = part + yrecv[k, Z_OWN, :, here].astype(F32)
        came(zrecv.at[pl.ds(1, nz - 2), :, at], z_rs.at[c])
        for p in range(1, nz - 1):
            part = part + zrecv[p, :, here].astype(F32)
        tg_ref[yi, zi, :, here] = part.astype(BF16)
        ref = tg_ref.at[yi, zi, :, at]
        for r, (p0, p1) in enumerate(Z_RUNS):
            for p in range(p0, p1):
                rcopy(ref, ref, s_az, az_rs.at[c * runs + r], z_dev(Z_ORDER[p])).start()
        for k in Y_ORDER:
            rcopy(ref, ref, s_ay, yo_rs.at[CHUNKS + c], y_dev(k)).start()

    def to_far(c):
        here, at = cut(c)
        came(tg_ref.at[pl.ds(0, NY - 1), 0, :, at], yo_rs.at[CHUNKS + c])
        ref = tg_ref.at[:, zi, :, at]
        rcopy(ref, ref, s_az, far_rs.at[CHUNKS + c], z_dev(Z_ORDER[Z_FAR])).start()

    def pass_on(c, r):
        here, at = cut(c)
        p0, p1 = Z_RUNS[r]
        came(zrecv.at[pl.ds(p0, p1 - p0), :, at], az_rs.at[c * runs + r])
        for p in range(p0, p1):
            ref = tg_ref.at[yi, lax.rem(zi + nz - Z_ORDER[p], nz), :, at]
            for k in Y_ORDER:
                rcopy(ref, ref, s_ay, in_ay, y_dev(k)).start()

    over_y(0, 0)
    over_y(0, 1)
    over_y(0, 2)
    over_y(1, 0)
    over_far(0)
    over_y(1, 1)
    over_y(1, 2)
    over_far(1)
    leave(0)
    leave(1)
    to_far(0)
    pass_on(0, 2)
    pass_on(0, 1)
    to_far(1)
    pass_on(1, 2)
    pass_on(0, 0)
    pass_on(1, 1)
    pass_on(1, 0)
    for c in range(CHUNKS):
        here, at = cut(c)
        came(tg_ref.at[:, 0, :, at], far_rs.at[CHUNKS + c])
    others = pl.ds(0, nz - 2)
    came(tg_ref.at[pl.ds(0, NY - 1), others], in_ay)
    gone(ids_all.at[pl.ds(1, owners - 1)], s_ids)
    gone(rsend.at[pl.ds(1, owners - 1)], s_row)
    gone(gsend.at[pl.ds(1, owners - 1)], s_x)
    gone(ysend.at[pl.ds(1, NY - 1), pl.ds(0, nz - 1)], s_y)
    gone(zsend.at[pl.ds(0, nz - 2)], s_z)
    gone(tg_ref.at[:, 0], s_z)
    gone(zsend.at[pl.ds(0, nz - 2)], s_az)
    gone(tg_ref.at[:, 0], s_az)
    gone(tg_ref.at[pl.ds(0, NY - 1), pl.ds(0, nz - 1)], s_ay)


def deliver(mixed_ref, tg_ref, out_hbm, grad_hbm, wide, sem):
    first = pltpu.make_async_copy(mixed_ref, out_hbm, sem.at[0])
    first.start()
    rows = wide.shape[0] // DELIVERIES
    copies = []
    for i in range(DELIVERIES):
        at = slice(i * rows, (i + 1) * rows)
        wide[at, :] = tg_ref[at, :].astype(F32)
        c = pltpu.make_async_copy(
            wide.at[pl.ds(i * rows, rows)], grad_hbm.at[pl.ds(i * rows, rows)], sem.at[i + 1]
        )
        c.start()
        copies.append(c)
    first.wait()
    for c in copies:
        c.wait()


def solution(mesh):
    owners = mesh.shape["rows"]
    nz = mesh.shape["dp"] // NY

    def shards(item_ids, lengths, item_table, in_weight, out_weight, grad_out):
        tokens = item_ids.shape[0]
        shard_rows, features = item_table.shape
        cap = 2 * tokens // owners
        piece = shard_rows // (NY * nz)
        dma = pltpu.SemaphoreType.DMA
        any_spec = pl.BlockSpec(memory_space=pl.ANY)
        vmem = pl.BlockSpec(memory_space=pltpu.VMEM)
        heads2 = HEADS // 2
        mixed, table_grad = pl.pallas_call(
            functools.partial(kernel, owners, nz),
            name="hstu",
            out_shape=(
                jax.ShapeDtypeStruct((tokens, features), BF16),
                jax.ShapeDtypeStruct((NY, nz, piece, features), BF16),
            ),
            in_specs=[any_spec] * 6,
            out_specs=(vmem, vmem),
            scratch_shapes=[
                pltpu.VMEM((1, tokens), I32),
                pltpu.VMEM((owners, 1, tokens), I32),
                pltpu.SMEM(lengths.shape, I32),
                pltpu.VMEM((shard_rows, features), BF16),
                pltpu.VMEM(in_weight.shape, BF16),
                pltpu.VMEM(out_weight.shape, BF16),
                pltpu.VMEM((tokens, features), BF16),
                pltpu.VMEM((owners, cap, features), BF16),
                pltpu.VMEM((owners, cap, features), BF16),
                pltpu.VMEM((shard_rows, owners * cap), BF16),
                pltpu.VMEM((owners * cap, tokens), BF16),
                pltpu.VMEM((tokens, owners * cap), BF16),
                pltpu.VMEM((tokens, features), F32),
                pltpu.VMEM((tokens, tokens), F32),
                pltpu.VMEM((tokens, 4 * features), F32),
                pltpu.VMEM((tokens, features), F32),
                pltpu.VMEM((tokens, 3 * features), BF16),
                pltpu.VMEM((heads2, 2 * tokens, tokens), BF16),
                pltpu.VMEM((heads2, 2 * tokens, tokens), F32),
                pltpu.VMEM((tokens, features), F32),
                pltpu.VMEM((tokens, 4 * features), BF16),
                pltpu.VMEM((owners, cap, features), BF16),
                pltpu.VMEM((owners, cap, features), BF16),
                pltpu.VMEM((NY, nz, piece, features), BF16),
                pltpu.VMEM((NY, nz, piece, features), BF16),
                pltpu.VMEM((nz, piece, features), BF16),
                pltpu.VMEM((nz, piece, features), BF16),
                pltpu.VMEM((piece, features), F32),
                pltpu.VMEM((NY, piece, features), BF16),
                pltpu.VMEM((NY, piece, features), BF16),
                dma((6,)),
                dma((7,)),
                dma((3,)),
                dma((CHUNKS,)),
                dma((CHUNKS * len(Z_RUNS),)),
                dma((CHUNKS,)),
                dma((CHUNKS * len(Z_RUNS),)),
                dma((2 * CHUNKS,)),
                dma((2 * CHUNKS,)),
                pltpu.SemaphoreType.REGULAR,
                pltpu.SemaphoreType.REGULAR,
            ],
            compiler_params=pltpu.CompilerParams(
                collective_id=0, has_side_effects=True, vmem_limit_bytes=40 * 1024 * 1024
            ),
        )(
            *[
                pltpu.with_memory_space_constraint(v, pltpu.HBM)
                for v in (item_ids.reshape(1, tokens), lengths, item_table, in_weight, out_weight, grad_out)
            ]
        )
        return pl.pallas_call(
            deliver,
            name="deliver",
            out_shape=(
                jax.ShapeDtypeStruct((tokens, features), BF16),
                jax.ShapeDtypeStruct((shard_rows, features), F32),
            ),
            in_specs=[vmem, vmem],
            out_specs=(any_spec, any_spec),
            scratch_shapes=[pltpu.VMEM((shard_rows, features), F32), dma((DELIVERIES + 1,))],
            compiler_params=pltpu.CompilerParams(vmem_limit_bytes=8 * 1024 * 1024),
        )(mixed, table_grad.reshape(shard_rows, features))

    return jax.shard_map(
        shards,
        mesh=mesh,
        in_specs=(
            P(("dp", "rows")),
            P(("dp", "rows"), None),
            P("rows", None),
            P(),
            P(),
            P(("dp", "rows"), None),
        ),
        out_specs=(P(("dp", "rows"), None), P("rows", None)),
        check_vma=False,
    )
```

```python
import functools

import jax
import jax.numpy as jnp
from jax import lax
from jax.experimental import pallas as pl
from jax.experimental.pallas import tpu as pltpu
from jax.sharding import PartitionSpec as P

HEADS = 8
MAXLEN = 64
EPS = 1e-06
NY = 4
CHUNKS = 2
DELIVERIES = 4
F32 = jnp.float32
BF16 = jnp.bfloat16
I32 = jnp.int32
ROW_ORDER = (4, 3, 5, 2, 6, 1, 7)
Y_ORDER = (2, 1, 3)
Z_ORDER = (4, 3, 5, 2, 6, 1, 7, 0)
Z_FAR, Z_OWN = 0, 7
Z_RUNS = ((1, 3), (3, 5), (5, 7))
MESH = pl.DeviceIdType.MESH


def mm(left, right):
    return jnp.dot(left, right, preferred_element_type=F32)


def mm_last(left, right):
    return lax.dot_general(left, right, (((1,), (1,)), ((), ())), preferred_element_type=F32)


def mm_first(left, right):
    return lax.dot_general(left, right, (((0,), (0,)), ((), ())), preferred_element_type=F32)


def sigmoid(v):
    return 0.5 * jnp.tanh(0.5 * v) + 0.5


def iota(shape, dim):
    return lax.broadcasted_iota(I32, shape, dim)


def kernel(
    owners,
    nz,
    ids_hbm,
    lens_hbm,
    table_hbm,
    win_hbm,
    wout_hbm,
    cot_hbm,
    out_ref,
    tg_ref,
    ids_v,
    note_s,
    ids_all,
    lens_s,
    tab,
    win,
    win_t,
    wout,
    cot_v,
    rsend,
    fetched,
    at_s,
    pt_s,
    p_s,
    gg_s,
    allow_s,
    dact_s,
    gate_s,
    vqk_s,
    w_s,
    dsw_s,
    att_s,
    gpre_s,
    gsend,
    grecv,
    ysend,
    yrecv,
    zsend,
    zrecv,
    own_s,
    far_in,
    own_send,
    local_sem,
    send_sem,
    in_sem,
    x_rs,
    y_rs,
    z_rs,
    az_rs,
    far_rs,
    yo_rs,
    near_sem,
    far_sem,
):
    tokens = ids_v.shape[1]
    shard_rows, features = tab.shape
    cap = rsend.shape[1]
    piece = zsend.shape[1]
    cw = features // CHUNKS
    me = lax.axis_index("rows")
    dp = lax.axis_index("dp")
    yi = dp // nz
    zi = lax.rem(dp, nz)

    def row_dev(k):
        return (dp, lax.rem(me + owners - k, owners))

    def y_of(k):
        return lax.rem(yi + k, NY)

    def z_of(k):
        return lax.rem(zi + k, nz)

    def y_dev(k):
        return (y_of(k) * nz + zi, me)

    def z_dev(k):
        return (yi * nz + z_of(k), me)

    def rcopy(src, dst, ss, rs, dev):
        return pltpu.make_async_remote_copy(
            src_ref=src, dst_ref=dst, send_sem=ss, recv_sem=rs, device_id=dev, device_id_type=MESH
        )

    def signal(sem, dev):
        pl.semaphore_signal(sem, inc=1, device_id=dev, device_id_type=MESH)

    s_ids, s_row, s_x, s_y, s_z, s_az, s_ay = (send_sem.at[i] for i in range(7))
    in_ids, in_row, in_ay = (in_sem.at[i] for i in range(3))

    def came(ref, sem):
        rcopy(ref, ref, s_ids, sem, row_dev(1)).wait_recv()

    def gone(ref, sem):
        rcopy(ref, ref, sem, in_ids, row_dev(1)).wait_send()

    ids_load = pltpu.make_async_copy(ids_hbm, ids_v, local_sem.at[0])
    lens_load = pltpu.make_async_copy(lens_hbm, lens_s, local_sem.at[1])
    tab_load = pltpu.make_async_copy(table_hbm, tab, local_sem.at[2])
    win_load = pltpu.make_async_copy(win_hbm, win, local_sem.at[3])
    wout_load = pltpu.make_async_copy(wout_hbm, wout, local_sem.at[4])
    cot_load = pltpu.make_async_copy(cot_hbm, cot_v, local_sem.at[5])
    ids_load.start()

    barrier = pltpu.get_barrier_semaphore()
    for k in ROW_ORDER:
        signal(barrier, row_dev(k))
    for k in (1, NY - 1):
        signal(barrier, y_dev(k))
    for k in (1, nz - 1):
        signal(barrier, z_dev(k))
    tab_load.start()
    lens_load.start()
    cot_load.start()
    wout_load.start()
    win_load.start()
    ids_load.wait()
    ids = ids_v[...]
    before = (iota((tokens, tokens), 0) < iota((tokens, tokens), 1)).astype(BF16)
    rel = lax.rem(me + owners - ids // shard_rows, owners)
    memb = rel == iota((owners, tokens), 0)
    rank = jnp.sum(jnp.where(memb, mm(memb.astype(BF16), before), 0.0), axis=0, keepdims=True)
    note_s[0:1, :] = ids
    note_s[1:2, :] = rank.astype(I32)
    pl.semaphore_wait(barrier, len(ROW_ORDER) + 4)

    for k in ROW_ORDER:
        rcopy(note_s, ids_all.at[owners - k], s_ids, in_ids, row_dev(k)).start()
    for k in (1, nz - 1):
        signal(near_sem, z_dev(k))
    for k in (1, NY - 1):
        signal(near_sem, y_dev(k))

    slot_row = rank + (rel * cap).astype(F32)
    slot_ids = iota((owners * cap, tokens), 0).astype(F32)
    pt_s[...] = (slot_ids == slot_row).astype(BF16)
    diag = iota((tokens, tokens), 0) == iota((tokens, tokens), 1)
    slot_col = jnp.sum(
        jnp.where(diag, jnp.broadcast_to(slot_row, (tokens, tokens)), 0.0), axis=1, keepdims=True
    )
    p_s[...] = (iota((tokens, owners * cap), 1).astype(F32) == slot_col).astype(BF16)

    lens_load.wait()
    ends = []
    total = lens_s[0, 0]
    ends.append(total)
    for u in range(1, lens_s.shape[1]):
        total = total + lens_s[0, u]
        ends.append(total)
    ti = iota((tokens, tokens), 0)
    tj = iota((tokens, tokens), 1)
    ui = sum((ti >= e).astype(I32) for e in ends)
    uj = sum((tj >= e).astype(I32) for e in ends)
    allow_s[...] = jnp.where((ui == uj) & (tj <= ti), 1.0 / MAXLEN, 0.0)

    came(ids_all.at[pl.ds(1, owners - 1)], in_ids)
    lo = me * shard_rows
    slots = iota((cap, tokens), 0)
    cols = []
    for k in range(owners):
        note = note_s[...] if k == 0 else ids_all[k]
        asked, place = note[0:1, :], note[1:2, :]
        mine = (asked >= lo) & (asked < lo + shard_rows)
        key = jnp.where(mine, place, -1)
        off1 = jnp.where(mine, asked - lo + 1, 0).astype(F32)
        cols.append(jnp.sum(jnp.where(slots == key, off1, 0.0), axis=1, keepdims=True))
    off_col = jnp.concatenate(cols, axis=0) - 1.0
    pick = (iota((owners * cap, shard_rows), 1).astype(F32) == off_col).astype(BF16)
    tab_load.wait()
    found = mm(pick, tab[...]).astype(BF16)
    rsend[...] = found.reshape(owners, cap, features)
    for k in ROW_ORDER:
        rcopy(rsend.at[k], fetched.at[owners - k], s_row, in_row, row_dev(k)).start()
    fetched[0] = rsend[0]

    spot = iota((1, shard_rows), 1)
    run_at = lax.rem(spot // piece, nz)
    along_z = sum(jnp.where(run_at == i, z, 0) for i, z in enumerate(Z_ORDER))
    item = (
        lax.rem(yi + spot // (piece * nz), NY) * (piece * nz)
        + lax.rem(zi + along_z, nz) * piece
        + lax.rem(spot, piece)
    )
    at_s[...] = (item.astype(F32) == off_col).astype(BF16).T
    cot_load.wait()
    wout_load.wait()
    gg_s[...] = mm_last(cot_v[...], wout[...])
    win_load.wait()
    for j in range(4):
        win_t[j * features : (j + 1) * features, :] = win[:, j * features : (j + 1) * features].T
    pl.semaphore_wait(near_sem, 4)
    for k in (2, nz - 2):
        signal(far_sem, z_dev(k))

    came(fetched.at[pl.ds(1, owners - 1)], in_row)
    x = mm(p_s[...], fetched[...].reshape(owners * cap, features))
    half = x.astype(BF16)
    row_scale = lax.rsqrt(jnp.mean(x * x, axis=-1, keepdims=True) + EPS)
    width = 256
    for j in range(4 * features // width):
        here = slice(j * width, (j + 1) * width)
        p = mm(half, win[:, here]) * row_scale
        s = sigmoid(p)
        a = p * s
        dact_s[:, here] = s + a * (1.0 - s)
        if j * width < features:
            gate_s[:, here] = a
        else:
            vqk_s[:, j * width - features : (j + 1) * width - features] = a.astype(BF16)

    pair = 2 * (features // HEADS)
    low = iota((tokens, pair), 1) < pair // 2
    allow = allow_s[...]
    allow2 = jnp.concatenate([allow, allow], axis=0)
    zero = jnp.zeros((tokens, pair), BF16)

    def split(b):
        return jnp.concatenate([jnp.where(low, b, zero), jnp.where(low, zero, b)], axis=0)

    def beside(b):
        return jnp.concatenate([b[:tokens], b[tokens:]], axis=1)

    score_scale = (features // HEADS) ** (-0.5)
    for g in range(HEADS // 2):
        v2 = vqk_s[:, g * pair : (g + 1) * pair]
        q2 = vqk_s[:, features + g * pair : features + (g + 1) * pair]
        k2 = vqk_s[:, 2 * features + g * pair : 2 * features + (g + 1) * pair]
        s = mm_last(split(q2), k2) * score_scale
        sg = sigmoid(s)
        w = (s * sg * allow2).astype(BF16)
        w_s[g] = w
        dsw_s[g] = allow2 * sg * (1.0 + s * (1.0 - sg)) * score_scale
        att_s[:, g * pair : (g + 1) * pair] = mm(beside(w), split(v2))

    att = att_s[...]
    gate = gate_s[...]
    gg = gg_s[...]
    grad_unit = gg * gate
    dot_o = jnp.mean(grad_unit * att, axis=-1, keepdims=True)
    att_scale = lax.rsqrt(jnp.mean(att * att, axis=-1, keepdims=True) + EPS)
    unit_o = att * att_scale
    ga = att_scale * (grad_unit - unit_o * (att_scale * dot_o))
    ga = ga.astype(BF16)
    gpre_s[:, :features] = (gg * unit_o * dact_s[:, :features]).astype(BF16)
    gated = (unit_o * gate).astype(BF16)
    for g in range(HEADS // 2):
        v_at = slice(features + g * pair, features + (g + 1) * pair)
        q_at = slice(2 * features + g * pair, 2 * features + (g + 1) * pair)
        k_at = slice(3 * features + g * pair, 3 * features + (g + 1) * pair)
        v2 = vqk_s[:, g * pair : (g + 1) * pair]
        q2 = vqk_s[:, features + g * pair : features + (g + 1) * pair]
        k2 = vqk_s[:, 2 * features + g * pair : 2 * features + (g + 1) * pair]
        gas = split(ga[:, g * pair : (g + 1) * pair])
        gw = mm_last(gas, v2)
        ds = (gw * dsw_s[g]).astype(BF16)
        gv = mm_first(w_s[g], gas)
        gq = mm(beside(ds), split(k2))
        gk = mm_first(ds, split(q2))
        gpre_s[:, v_at] = (gv * dact_s[:, v_at]).astype(BF16)
        gpre_s[:, q_at] = (gq * dact_s[:, q_at]).astype(BF16)
        gpre_s[:, k_at] = (gk * dact_s[:, k_at]).astype(BF16)
    unit_x = x * row_scale
    gn = mm(gpre_s[...], win_t[...])
    grad_rows = cot_v[...].astype(F32) + row_scale * (
        gn - unit_x * jnp.mean(gn * unit_x, axis=-1, keepdims=True)
    )
    grad_rows = grad_rows.astype(BF16)
    for c in range(CHUNKS):
        here = slice(c * cw, (c + 1) * cw)
        at = pl.ds(c * cw, cw)
        outgoing = mm(pt_s[...], grad_rows[:, here]).astype(BF16)
        gsend[:, :, here] = outgoing.reshape(owners, cap, cw)
        for k in ROW_ORDER:
            rcopy(gsend.at[k, :, at], grecv.at[owners - k, :, at], s_x, x_rs.at[c], row_dev(k)).start()
    grecv[0] = gsend[0]

    out_ref[...] = (x + mm(gated, wout[...])).astype(BF16)
    pl.semaphore_wait(far_sem, 2)

    runs = len(Z_RUNS)

    def cut(c):
        return slice(c * cw, (c + 1) * cw), pl.ds(c * cw, cw)

    for c in range(CHUNKS):
        here, at = cut(c)
        came(grecv.at[pl.ds(1, owners - 1), :, at], x_rs.at[c])
        dense = mm(at_s[...], grecv[:, :, here].reshape(owners * cap, cw)).astype(BF16)
        ysend[:, :, :, here] = dense.reshape(NY, nz, piece, cw)
        rcopy(
            ysend.at[:, Z_FAR, :, at],
            far_in.at[:, :, at],
            s_z,
            far_rs.at[c],
            z_dev(Z_ORDER[Z_FAR]),
        ).start()
        for r, (p0, p1) in enumerate(Z_RUNS):
            run = pl.ds(p0, p1 - p0)
            for k in Y_ORDER:
                rcopy(
                    ysend.at[k, run, :, at],
                    yrecv.at[k, run, :, at],
                    s_y,
                    y_rs.at[c * runs + r],
                    y_dev(k),
                ).start()

    def over_y(c, r):
        here, at = cut(c)
        p0, p1 = Z_RUNS[r]
        came(yrecv.at[pl.ds(1, NY - 1), pl.ds(p0, p1 - p0), :, at], y_rs.at[c * runs + r])
        part = ysend[0, p0:p1, :, here].astype(F32)
        for k in range(1, NY):
            part = part + yrecv[k, p0:p1, :, here].astype(F32)
        zsend[p0:p1, :, here] = part.astype(BF16)
        for p in range(p0, p1):
            rcopy(
                zsend.at[p, :, at], zrecv.at[p, :, at], s_z, z_rs.at[c], z_dev(Z_ORDER[p])
            ).start()

    def over_far(c):
        here, at = cut(c)
        came(far_in.at[:, :, at], far_rs.at[c])
        part = ysend[:, Z_OWN, :, here].astype(F32) + far_in[:, :, here].astype(F32)
        own_s[:, here] = part[0]
        own_send[:, :, here] = part.astype(BF16)
        for k in Y_ORDER:
            rcopy(
                own_send.at[k, :, at], yrecv.at[k, Z_OWN, :, at], s_y, yo_rs.at[c], y_dev(k)
            ).start()

    def leave(c):
        here, at = cut(c)
        came(yrecv.at[pl.ds(1, NY - 1), Z_OWN, :, at], yo_rs.at[c])
        part = own_s[:, here]
        for k in range(1, NY):
            part = part + yrecv[k, Z_OWN, :, here].astype(F32)
        came(zrecv.at[pl.ds(1, nz - 2), :, at], z_rs.at[c])
        for p in range(1, nz - 1):
            part = part + zrecv[p, :, here].astype(F32)
        tg_ref[yi, zi, :, here] = part.astype(BF16)
        ref = tg_ref.at[yi, zi, :, at]
        for r, (p0, p1) in enumerate(Z_RUNS):
            for p in range(p0, p1):
                rcopy(ref, ref, s_az, az_rs.at[c * runs + r], z_dev(Z_ORDER[p])).start()
        for k in Y_ORDER:
            rcopy(ref, ref, s_ay, yo_rs.at[CHUNKS + c], y_dev(k)).start()

    def to_far(c):
        here, at = cut(c)
        came(tg_ref.at[pl.ds(0, NY - 1), 0, :, at], yo_rs.at[CHUNKS + c])
        ref = tg_ref.at[:, zi, :, at]
        rcopy(ref, ref, s_az, far_rs.at[CHUNKS + c], z_dev(Z_ORDER[Z_FAR])).start()

    def pass_on(c, r):
        here, at = cut(c)
        p0, p1 = Z_RUNS[r]
        came(zrecv.at[pl.ds(p0, p1 - p0), :, at], az_rs.at[c * runs + r])
        for p in range(p0, p1):
            ref = tg_ref.at[yi, lax.rem(zi + nz - Z_ORDER[p], nz), :, at]
            for k in Y_ORDER:
                rcopy(ref, ref, s_ay, in_ay, y_dev(k)).start()

    over_y(0, 0)
    over_y(0, 1)
    over_y(0, 2)
    over_y(1, 0)
    over_far(0)
    over_y(1, 1)
    over_y(1, 2)
    over_far(1)
    leave(0)
    leave(1)
    to_far(0)
    pass_on(0, 2)
    pass_on(0, 1)
    to_far(1)
    pass_on(1, 2)
    pass_on(0, 0)
    pass_on(1, 1)
    pass_on(1, 0)
    for c in range(CHUNKS):
        here, at = cut(c)
        came(tg_ref.at[:, 0, :, at], far_rs.at[CHUNKS + c])
    others = pl.ds(0, nz - 2)
    came(tg_ref.at[pl.ds(0, NY - 1), others], in_ay)
    gone(ids_all.at[pl.ds(1, owners - 1)], s_ids)
    gone(rsend.at[pl.ds(1, owners - 1)], s_row)
    gone(gsend.at[pl.ds(1, owners - 1)], s_x)
    gone(ysend.at[pl.ds(1, NY - 1), pl.ds(0, nz - 1)], s_y)
    gone(zsend.at[pl.ds(0, nz - 2)], s_z)
    gone(tg_ref.at[:, 0], s_z)
    gone(zsend.at[pl.ds(0, nz - 2)], s_az)
    gone(tg_ref.at[:, 0], s_az)
    gone(tg_ref.at[pl.ds(0, NY - 1), pl.ds(0, nz - 1)], s_ay)


def deliver(mixed_ref, tg_ref, out_hbm, grad_hbm, wide, sem):
    first = pltpu.make_async_copy(mixed_ref, out_hbm, sem.at[0])
    first.start()
    rows = wide.shape[0] // DELIVERIES
    copies = []
    for i in range(DELIVERIES):
        at = slice(i * rows, (i + 1) * rows)
        wide[at, :] = tg_ref[at, :].astype(F32)
        c = pltpu.make_async_copy(
            wide.at[pl.ds(i * rows, rows)], grad_hbm.at[pl.ds(i * rows, rows)], sem.at[i + 1]
        )
        c.start()
        copies.append(c)
    first.wait()
    for c in copies:
        c.wait()


def solution(mesh):
    owners = mesh.shape["rows"]
    nz = mesh.shape["dp"] // NY

    def shards(item_ids, lengths, item_table, in_weight, out_weight, grad_out):
        tokens = item_ids.shape[0]
        shard_rows, features = item_table.shape
        cap = 2 * tokens // owners
        piece = shard_rows // (NY * nz)
        dma = pltpu.SemaphoreType.DMA
        any_spec = pl.BlockSpec(memory_space=pl.ANY)
        vmem = pl.BlockSpec(memory_space=pltpu.VMEM)
        heads2 = HEADS // 2
        mixed, table_grad = pl.pallas_call(
            functools.partial(kernel, owners, nz),
            name="hstu",
            out_shape=(
                jax.ShapeDtypeStruct((tokens, features), BF16),
                jax.ShapeDtypeStruct((NY, nz, piece, features), BF16),
            ),
            in_specs=[any_spec] * 6,
            out_specs=(vmem, vmem),
            scratch_shapes=[
                pltpu.VMEM((1, tokens), I32),
                pltpu.VMEM((2, tokens), I32),
                pltpu.VMEM((owners, 2, tokens), I32),
                pltpu.SMEM(lengths.shape, I32),
                pltpu.VMEM((shard_rows, features), BF16),
                pltpu.VMEM(in_weight.shape, BF16),
                pltpu.VMEM(in_weight.shape[::-1], BF16),
                pltpu.VMEM(out_weight.shape, BF16),
                pltpu.VMEM((tokens, features), BF16),
                pltpu.VMEM((owners, cap, features), BF16),
                pltpu.VMEM((owners, cap, features), BF16),
                pltpu.VMEM((shard_rows, owners * cap), BF16),
                pltpu.VMEM((owners * cap, tokens), BF16),
                pltpu.VMEM((tokens, owners * cap), BF16),
                pltpu.VMEM((tokens, features), F32),
                pltpu.VMEM((tokens, tokens), F32),
                pltpu.VMEM((tokens, 4 * features), F32),
                pltpu.VMEM((tokens, features), F32),
                pltpu.VMEM((tokens, 3 * features), BF16),
                pltpu.VMEM((heads2, 2 * tokens, tokens), BF16),
                pltpu.VMEM((heads2, 2 * tokens, tokens), F32),
                pltpu.VMEM((tokens, features), F32),
                pltpu.VMEM((tokens, 4 * features), BF16),
                pltpu.VMEM((owners, cap, features), BF16),
                pltpu.VMEM((owners, cap, features), BF16),
                pltpu.VMEM((NY, nz, piece, features), BF16),
                pltpu.VMEM((NY, nz, piece, features), BF16),
                pltpu.VMEM((nz, piece, features), BF16),
                pltpu.VMEM((nz, piece, features), BF16),
                pltpu.VMEM((piece, features), F32),
                pltpu.VMEM((NY, piece, features), BF16),
                pltpu.VMEM((NY, piece, features), BF16),
                dma((6,)),
                dma((7,)),
                dma((3,)),
                dma((CHUNKS,)),
                dma((CHUNKS * len(Z_RUNS),)),
                dma((CHUNKS,)),
                dma((CHUNKS * len(Z_RUNS),)),
                dma((2 * CHUNKS,)),
                dma((2 * CHUNKS,)),
                pltpu.SemaphoreType.REGULAR,
                pltpu.SemaphoreType.REGULAR,
            ],
            compiler_params=pltpu.CompilerParams(
                collective_id=0, has_side_effects=True, vmem_limit_bytes=40 * 1024 * 1024
            ),
        )(
            *[
                pltpu.with_memory_space_constraint(v, pltpu.HBM)
                for v in (item_ids.reshape(1, tokens), lengths, item_table, in_weight, out_weight, grad_out)
            ]
        )
        return pl.pallas_call(
            deliver,
            name="deliver",
            out_shape=(
                jax.ShapeDtypeStruct((tokens, features), BF16),
                jax.ShapeDtypeStruct((shard_rows, features), F32),
            ),
            in_specs=[vmem, vmem],
            out_specs=(any_spec, any_spec),
            scratch_shapes=[pltpu.VMEM((shard_rows, features), F32), dma((DELIVERIES + 1,))],
            compiler_params=pltpu.CompilerParams(vmem_limit_bytes=8 * 1024 * 1024),
        )(mixed, table_grad.reshape(shard_rows, features))

    return jax.shard_map(
        shards,
        mesh=mesh,
        in_specs=(
            P(("dp", "rows")),
            P(("dp", "rows"), None),
            P("rows", None),
            P(),
            P(),
            P(("dp", "rows"), None),
        ),
        out_specs=(P(("dp", "rows"), None), P("rows", None)),
        check_vma=False,
    )
```

```python
import functools

import jax
import jax.numpy as jnp
from jax import lax
from jax.experimental import pallas as pl
from jax.experimental.pallas import tpu as pltpu
from jax.sharding import PartitionSpec as P

HEADS = 8
MAXLEN = 64
EPS = 1e-06
NY = 4
CUTS = ((0, 128), (128, 256), (256, 512))
CHUNKS = len(CUTS)
DELIVERIES = 4
F32 = jnp.float32
BF16 = jnp.bfloat16
I32 = jnp.int32
ROW_ORDER = (4, 3, 5, 2, 6, 1, 7)
Y_ORDER = (2, 1, 3)
Z_ORDER = (4, 3, 5, 2, 6, 1, 7, 0)
Z_FAR, Z_OWN = 0, 7
Z_RUNS = ((1, 3), (3, 5), (5, 7))
MESH = pl.DeviceIdType.MESH


def mm(left, right):
    return jnp.dot(left, right, preferred_element_type=F32)


def mm_last(left, right):
    return lax.dot_general(left, right, (((1,), (1,)), ((), ())), preferred_element_type=F32)


def mm_first(left, right):
    return lax.dot_general(left, right, (((0,), (0,)), ((), ())), preferred_element_type=F32)


def sigmoid(v):
    return 0.5 * jnp.tanh(0.5 * v) + 0.5


def iota(shape, dim):
    return lax.broadcasted_iota(I32, shape, dim)


def kernel(
    owners,
    nz,
    ids_hbm,
    lens_hbm,
    table_hbm,
    win_hbm,
    wout_hbm,
    cot_hbm,
    out_ref,
    tg_ref,
    ids_v,
    note_s,
    ids_all,
    lens_s,
    tab,
    win,
    win_t,
    wout,
    cot_v,
    rsend,
    fetched,
    at_s,
    pt_s,
    p_s,
    gg_s,
    allow_s,
    dact_s,
    gate_s,
    vqk_s,
    w_s,
    dsw_s,
    att_s,
    gpre_s,
    gsend,
    grecv,
    ysend,
    yrecv,
    zsend,
    zrecv,
    own_s,
    far_in,
    own_send,
    local_sem,
    send_sem,
    in_sem,
    x_rs,
    y_rs,
    z_rs,
    az_rs,
    far_rs,
    yo_rs,
    near_sem,
    far_sem,
):
    tokens = ids_v.shape[1]
    shard_rows, features = tab.shape
    cap = rsend.shape[1]
    piece = zsend.shape[1]
    me = lax.axis_index("rows")
    dp = lax.axis_index("dp")
    yi = dp // nz
    zi = lax.rem(dp, nz)

    def row_dev(k):
        return (dp, lax.rem(me + owners - k, owners))

    def y_of(k):
        return lax.rem(yi + k, NY)

    def z_of(k):
        return lax.rem(zi + k, nz)

    def y_dev(k):
        return (y_of(k) * nz + zi, me)

    def z_dev(k):
        return (yi * nz + z_of(k), me)

    def rcopy(src, dst, ss, rs, dev):
        return pltpu.make_async_remote_copy(
            src_ref=src, dst_ref=dst, send_sem=ss, recv_sem=rs, device_id=dev, device_id_type=MESH
        )

    def signal(sem, dev):
        pl.semaphore_signal(sem, inc=1, device_id=dev, device_id_type=MESH)

    s_ids, s_row, s_x, s_y, s_z, s_az, s_ay = (send_sem.at[i] for i in range(7))
    in_ids, in_row, in_ay = (in_sem.at[i] for i in range(3))

    def came(ref, sem):
        rcopy(ref, ref, s_ids, sem, row_dev(1)).wait_recv()

    def gone(ref, sem):
        rcopy(ref, ref, sem, in_ids, row_dev(1)).wait_send()

    ids_load = pltpu.make_async_copy(ids_hbm, ids_v, local_sem.at[0])
    lens_load = pltpu.make_async_copy(lens_hbm, lens_s, local_sem.at[1])
    tab_load = pltpu.make_async_copy(table_hbm, tab, local_sem.at[2])
    win_load = pltpu.make_async_copy(win_hbm, win, local_sem.at[3])
    wout_load = pltpu.make_async_copy(wout_hbm, wout, local_sem.at[4])
    cot_load = pltpu.make_async_copy(cot_hbm, cot_v, local_sem.at[5])
    ids_load.start()

    barrier = pltpu.get_barrier_semaphore()
    for k in ROW_ORDER:
        signal(barrier, row_dev(k))
    for k in (1, NY - 1):
        signal(barrier, y_dev(k))
    for k in (1, nz - 1):
        signal(barrier, z_dev(k))
    tab_load.start()
    lens_load.start()
    cot_load.start()
    wout_load.start()
    win_load.start()
    ids_load.wait()
    ids = ids_v[...]
    before = (iota((tokens, tokens), 0) < iota((tokens, tokens), 1)).astype(BF16)
    rel = lax.rem(me + owners - ids // shard_rows, owners)
    memb = rel == iota((owners, tokens), 0)
    rank = jnp.sum(jnp.where(memb, mm(memb.astype(BF16), before), 0.0), axis=0, keepdims=True)
    note_s[0:1, :] = ids
    note_s[1:2, :] = rank.astype(I32)
    pl.semaphore_wait(barrier, len(ROW_ORDER) + 4)

    for k in ROW_ORDER:
        rcopy(note_s, ids_all.at[owners - k], s_ids, in_ids, row_dev(k)).start()
    for k in (1, nz - 1):
        signal(near_sem, z_dev(k))
    for k in (1, NY - 1):
        signal(near_sem, y_dev(k))

    slot_row = rank + (rel * cap).astype(F32)
    slot_ids = iota((owners * cap, tokens), 0).astype(F32)
    pt_s[...] = (slot_ids == slot_row).astype(BF16)
    diag = iota((tokens, tokens), 0) == iota((tokens, tokens), 1)
    slot_col = jnp.sum(
        jnp.where(diag, jnp.broadcast_to(slot_row, (tokens, tokens)), 0.0), axis=1, keepdims=True
    )
    p_s[...] = (iota((tokens, owners * cap), 1).astype(F32) == slot_col).astype(BF16)

    lens_load.wait()
    ends = []
    total = lens_s[0, 0]
    ends.append(total)
    for u in range(1, lens_s.shape[1]):
        total = total + lens_s[0, u]
        ends.append(total)
    ti = iota((tokens, tokens), 0)
    tj = iota((tokens, tokens), 1)
    ui = sum((ti >= e).astype(I32) for e in ends)
    uj = sum((tj >= e).astype(I32) for e in ends)
    allow_s[...] = jnp.where((ui == uj) & (tj <= ti), 1.0 / MAXLEN, 0.0)

    came(ids_all.at[pl.ds(1, owners - 1)], in_ids)
    lo = me * shard_rows
    slots = iota((cap, tokens), 0)
    cols = []
    for k in range(owners):
        note = note_s[...] if k == 0 else ids_all[k]
        asked, place = note[0:1, :], note[1:2, :]
        mine = (asked >= lo) & (asked < lo + shard_rows)
        key = jnp.where(mine, place, -1)
        off1 = jnp.where(mine, asked - lo + 1, 0).astype(F32)
        cols.append(jnp.sum(jnp.where(slots == key, off1, 0.0), axis=1, keepdims=True))
    off_col = jnp.concatenate(cols, axis=0) - 1.0
    pick = (iota((owners * cap, shard_rows), 1).astype(F32) == off_col).astype(BF16)
    tab_load.wait()
    found = mm(pick, tab[...]).astype(BF16)
    rsend[...] = found.reshape(owners, cap, features)
    for k in ROW_ORDER:
        rcopy(rsend.at[k], fetched.at[owners - k], s_row, in_row, row_dev(k)).start()
    fetched[0] = rsend[0]

    spot = iota((1, shard_rows), 1)
    run_at = lax.rem(spot // piece, nz)
    along_z = sum(jnp.where(run_at == i, z, 0) for i, z in enumerate(Z_ORDER))
    item = (
        lax.rem(yi + spot // (piece * nz), NY) * (piece * nz)
        + lax.rem(zi + along_z, nz) * piece
        + lax.rem(spot, piece)
    )
    at_s[...] = (item.astype(F32) == off_col).astype(BF16).T
    cot_load.wait()
    wout_load.wait()
    gg_s[...] = mm_last(cot_v[...], wout[...])
    win_load.wait()
    for j in range(4):
        win_t[j * features : (j + 1) * features, :] = win[:, j * features : (j + 1) * features].T
    pl.semaphore_wait(near_sem, 4)
    for k in (2, nz - 2):
        signal(far_sem, z_dev(k))

    came(fetched.at[pl.ds(1, owners - 1)], in_row)
    x = mm(p_s[...], fetched[...].reshape(owners * cap, features))
    row_scale = lax.rsqrt(jnp.mean(x * x, axis=-1, keepdims=True) + EPS)
    normed = (x * row_scale).astype(BF16)
    width = 256
    for j in range(4 * features // width):
        here = slice(j * width, (j + 1) * width)
        p = mm(normed, win[:, here])
        s = sigmoid(p)
        a = p * s
        dact_s[:, here] = s + a * (1.0 - s)
        if j * width < features:
            gate_s[:, here] = a
        else:
            vqk_s[:, j * width - features : (j + 1) * width - features] = a.astype(BF16)

    pair = 2 * (features // HEADS)
    low = iota((tokens, pair), 1) < pair // 2
    allow = allow_s[...]
    allow2 = jnp.concatenate([allow, allow], axis=0)
    zero = jnp.zeros((tokens, pair), BF16)

    def split(b):
        return jnp.concatenate([jnp.where(low, b, zero), jnp.where(low, zero, b)], axis=0)

    def beside(b):
        return jnp.concatenate([b[:tokens], b[tokens:]], axis=1)

    score_scale = (features // HEADS) ** (-0.5)
    for g in range(HEADS // 2):
        v2 = vqk_s[:, g * pair : (g + 1) * pair]
        q2 = vqk_s[:, features + g * pair : features + (g + 1) * pair]
        k2 = vqk_s[:, 2 * features + g * pair : 2 * features + (g + 1) * pair]
        s = mm_last(split(q2), k2) * score_scale
        sg = sigmoid(s)
        w = (s * sg * allow2).astype(BF16)
        w_s[g] = w
        dsw_s[g] = allow2 * sg * (1.0 + s * (1.0 - sg)) * score_scale
        att_s[:, g * pair : (g + 1) * pair] = mm(beside(w), split(v2))

    att = att_s[...]
    gate = gate_s[...]
    gg = gg_s[...]
    grad_unit = gg * gate
    dot_o = jnp.mean(grad_unit * att, axis=-1, keepdims=True)
    att_scale = lax.rsqrt(jnp.mean(att * att, axis=-1, keepdims=True) + EPS)
    unit_o = att * att_scale
    ga = att_scale * (grad_unit - unit_o * (att_scale * dot_o))
    ga = ga.astype(BF16)
    gpre_s[:, :features] = (gg * unit_o * dact_s[:, :features]).astype(BF16)
    gated = (unit_o * gate).astype(BF16)
    for g in range(HEADS // 2):
        v_at = slice(features + g * pair, features + (g + 1) * pair)
        q_at = slice(2 * features + g * pair, 2 * features + (g + 1) * pair)
        k_at = slice(3 * features + g * pair, 3 * features + (g + 1) * pair)
        v2 = vqk_s[:, g * pair : (g + 1) * pair]
        q2 = vqk_s[:, features + g * pair : features + (g + 1) * pair]
        k2 = vqk_s[:, 2 * features + g * pair : 2 * features + (g + 1) * pair]
        gas = split(ga[:, g * pair : (g + 1) * pair])
        gw = mm_last(gas, v2)
        ds = (gw * dsw_s[g]).astype(BF16)
        gv = mm_first(w_s[g], gas)
        gq = mm(beside(ds), split(k2))
        gk = mm_first(ds, split(q2))
        gpre_s[:, v_at] = (gv * dact_s[:, v_at]).astype(BF16)
        gpre_s[:, q_at] = (gq * dact_s[:, q_at]).astype(BF16)
        gpre_s[:, k_at] = (gk * dact_s[:, k_at]).astype(BF16)
    unit_x = x * row_scale
    gn = mm(gpre_s[...], win_t[...])
    grad_rows = cot_v[...].astype(F32) + row_scale * (
        gn - unit_x * jnp.mean(gn * unit_x, axis=-1, keepdims=True)
    )
    grad_rows = grad_rows.astype(BF16)
    for c, (c0, c1) in enumerate(CUTS):
        here = slice(c0, c1)
        at = pl.ds(c0, c1 - c0)
        outgoing = mm(pt_s[...], grad_rows[:, here]).astype(BF16)
        gsend[:, :, here] = outgoing.reshape(owners, cap, c1 - c0)
        for k in ROW_ORDER:
            rcopy(gsend.at[k, :, at], grecv.at[owners - k, :, at], s_x, x_rs.at[c], row_dev(k)).start()
    grecv[0] = gsend[0]

    out_ref[...] = (x + mm(gated, wout[...])).astype(BF16)
    pl.semaphore_wait(far_sem, 2)

    runs = len(Z_RUNS)

    def cut(c):
        return slice(*CUTS[c]), pl.ds(CUTS[c][0], CUTS[c][1] - CUTS[c][0])

    for c in range(CHUNKS):
        here, at = cut(c)
        came(grecv.at[pl.ds(1, owners - 1), :, at], x_rs.at[c])
        dense = mm(at_s[...], grecv[:, :, here].reshape(owners * cap, -1)).astype(BF16)
        ysend[:, :, :, here] = dense.reshape(NY, nz, piece, -1)
        rcopy(
            ysend.at[:, Z_FAR, :, at],
            far_in.at[:, :, at],
            s_z,
            far_rs.at[c],
            z_dev(Z_ORDER[Z_FAR]),
        ).start()
        for r, (p0, p1) in enumerate(Z_RUNS):
            run = pl.ds(p0, p1 - p0)
            for k in Y_ORDER:
                rcopy(
                    ysend.at[k, run, :, at],
                    yrecv.at[k, run, :, at],
                    s_y,
                    y_rs.at[c * runs + r],
                    y_dev(k),
                ).start()

    def over_y(c, r):
        here, at = cut(c)
        p0, p1 = Z_RUNS[r]
        came(yrecv.at[pl.ds(1, NY - 1), pl.ds(p0, p1 - p0), :, at], y_rs.at[c * runs + r])
        part = ysend[0, p0:p1, :, here].astype(F32)
        for k in range(1, NY):
            part = part + yrecv[k, p0:p1, :, here].astype(F32)
        zsend[p0:p1, :, here] = part.astype(BF16)
        for p in range(p0, p1):
            rcopy(
                zsend.at[p, :, at], zrecv.at[p, :, at], s_z, z_rs.at[c], z_dev(Z_ORDER[p])
            ).start()

    def over_far(c):
        here, at = cut(c)
        came(far_in.at[:, :, at], far_rs.at[c])
        part = ysend[:, Z_OWN, :, here].astype(F32) + far_in[:, :, here].astype(F32)
        own_s[:, here] = part[0]
        own_send[:, :, here] = part.astype(BF16)
        for k in Y_ORDER:
            rcopy(
                own_send.at[k, :, at], yrecv.at[k, Z_OWN, :, at], s_y, yo_rs.at[c], y_dev(k)
            ).start()

    def leave(c):
        here, at = cut(c)
        came(yrecv.at[pl.ds(1, NY - 1), Z_OWN, :, at], yo_rs.at[c])
        part = own_s[:, here]
        for k in range(1, NY):
            part = part + yrecv[k, Z_OWN, :, here].astype(F32)
        came(zrecv.at[pl.ds(1, nz - 2), :, at], z_rs.at[c])
        for p in range(1, nz - 1):
            part = part + zrecv[p, :, here].astype(F32)
        tg_ref[yi, zi, :, here] = part.astype(BF16)
        ref = tg_ref.at[yi, zi, :, at]
        for r, (p0, p1) in enumerate(Z_RUNS):
            for p in range(p0, p1):
                rcopy(ref, ref, s_az, az_rs.at[c * runs + r], z_dev(Z_ORDER[p])).start()
        for k in Y_ORDER:
            rcopy(ref, ref, s_ay, yo_rs.at[CHUNKS + c], y_dev(k)).start()

    def to_far(c):
        here, at = cut(c)
        came(tg_ref.at[pl.ds(0, NY - 1), 0, :, at], yo_rs.at[CHUNKS + c])
        ref = tg_ref.at[:, zi, :, at]
        rcopy(ref, ref, s_az, far_rs.at[CHUNKS + c], z_dev(Z_ORDER[Z_FAR])).start()

    def pass_on(c, r):
        here, at = cut(c)
        p0, p1 = Z_RUNS[r]
        came(zrecv.at[pl.ds(p0, p1 - p0), :, at], az_rs.at[c * runs + r])
        for p in range(p0, p1):
            ref = tg_ref.at[yi, lax.rem(zi + nz - Z_ORDER[p], nz), :, at]
            for k in Y_ORDER:
                rcopy(ref, ref, s_ay, in_ay, y_dev(k)).start()

    for c in range(CHUNKS):
        for r in range(runs):
            over_y(c, r)
            if c > 0 and r == 0:
                over_far(c - 1)
    over_far(CHUNKS - 1)
    for c in range(CHUNKS):
        leave(c)
    steps = [(1.3 * c + 3.0, c, to_far) for c in range(CHUNKS)]
    for r, late in enumerate((4.6, 3.8, 3.1)):
        steps += [(1.3 * c + late, c, functools.partial(pass_on, r=r)) for c in range(CHUNKS)]
    for _, c, step in sorted(steps, key=lambda e: e[:2]):
        step(c)
    for c in range(CHUNKS):
        here, at = cut(c)
        came(tg_ref.at[:, 0, :, at], far_rs.at[CHUNKS + c])
    others = pl.ds(0, nz - 2)
    came(tg_ref.at[pl.ds(0, NY - 1), others], in_ay)
    gone(ids_all.at[pl.ds(1, owners - 1)], s_ids)
    gone(rsend.at[pl.ds(1, owners - 1)], s_row)
    gone(gsend.at[pl.ds(1, owners - 1)], s_x)
    gone(ysend.at[pl.ds(1, NY - 1), pl.ds(0, nz - 1)], s_y)
    gone(zsend.at[pl.ds(0, nz - 2)], s_z)
    gone(tg_ref.at[:, 0], s_z)
    gone(zsend.at[pl.ds(0, nz - 2)], s_az)
    gone(tg_ref.at[:, 0], s_az)
    gone(tg_ref.at[pl.ds(0, NY - 1), pl.ds(0, nz - 1)], s_ay)


def deliver(mixed_ref, tg_ref, out_hbm, grad_hbm, wide, sem):
    first = pltpu.make_async_copy(mixed_ref, out_hbm, sem.at[0])
    first.start()
    rows = wide.shape[0] // DELIVERIES
    copies = []
    for i in range(DELIVERIES):
        at = slice(i * rows, (i + 1) * rows)
        wide[at, :] = tg_ref[at, :].astype(F32)
        c = pltpu.make_async_copy(
            wide.at[pl.ds(i * rows, rows)], grad_hbm.at[pl.ds(i * rows, rows)], sem.at[i + 1]
        )
        c.start()
        copies.append(c)
    first.wait()
    for c in copies:
        c.wait()


def solution(mesh):
    owners = mesh.shape["rows"]
    nz = mesh.shape["dp"] // NY

    def shards(item_ids, lengths, item_table, in_weight, out_weight, grad_out):
        tokens = item_ids.shape[0]
        shard_rows, features = item_table.shape
        cap = 2 * tokens // owners
        piece = shard_rows // (NY * nz)
        dma = pltpu.SemaphoreType.DMA
        any_spec = pl.BlockSpec(memory_space=pl.ANY)
        vmem = pl.BlockSpec(memory_space=pltpu.VMEM)
        heads2 = HEADS // 2
        mixed, table_grad = pl.pallas_call(
            functools.partial(kernel, owners, nz),
            name="hstu",
            out_shape=(
                jax.ShapeDtypeStruct((tokens, features), BF16),
                jax.ShapeDtypeStruct((NY, nz, piece, features), BF16),
            ),
            in_specs=[any_spec] * 6,
            out_specs=(vmem, vmem),
            scratch_shapes=[
                pltpu.VMEM((1, tokens), I32),
                pltpu.VMEM((2, tokens), I32),
                pltpu.VMEM((owners, 2, tokens), I32),
                pltpu.SMEM(lengths.shape, I32),
                pltpu.VMEM((shard_rows, features), BF16),
                pltpu.VMEM(in_weight.shape, BF16),
                pltpu.VMEM(in_weight.shape[::-1], BF16),
                pltpu.VMEM(out_weight.shape, BF16),
                pltpu.VMEM((tokens, features), BF16),
                pltpu.VMEM((owners, cap, features), BF16),
                pltpu.VMEM((owners, cap, features), BF16),
                pltpu.VMEM((shard_rows, owners * cap), BF16),
                pltpu.VMEM((owners * cap, tokens), BF16),
                pltpu.VMEM((tokens, owners * cap), BF16),
                pltpu.VMEM((tokens, features), F32),
                pltpu.VMEM((tokens, tokens), F32),
                pltpu.VMEM((tokens, 4 * features), F32),
                pltpu.VMEM((tokens, features), F32),
                pltpu.VMEM((tokens, 3 * features), BF16),
                pltpu.VMEM((heads2, 2 * tokens, tokens), BF16),
                pltpu.VMEM((heads2, 2 * tokens, tokens), F32),
                pltpu.VMEM((tokens, features), F32),
                pltpu.VMEM((tokens, 4 * features), BF16),
                pltpu.VMEM((owners, cap, features), BF16),
                pltpu.VMEM((owners, cap, features), BF16),
                pltpu.VMEM((NY, nz, piece, features), BF16),
                pltpu.VMEM((NY, nz, piece, features), BF16),
                pltpu.VMEM((nz, piece, features), BF16),
                pltpu.VMEM((nz, piece, features), BF16),
                pltpu.VMEM((piece, features), F32),
                pltpu.VMEM((NY, piece, features), BF16),
                pltpu.VMEM((NY, piece, features), BF16),
                dma((6,)),
                dma((7,)),
                dma((3,)),
                dma((CHUNKS,)),
                dma((CHUNKS * len(Z_RUNS),)),
                dma((CHUNKS,)),
                dma((CHUNKS * len(Z_RUNS),)),
                dma((2 * CHUNKS,)),
                dma((2 * CHUNKS,)),
                pltpu.SemaphoreType.REGULAR,
                pltpu.SemaphoreType.REGULAR,
            ],
            compiler_params=pltpu.CompilerParams(
                collective_id=0, has_side_effects=True, vmem_limit_bytes=40 * 1024 * 1024
            ),
        )(
            *[
                pltpu.with_memory_space_constraint(v, pltpu.HBM)
                for v in (item_ids.reshape(1, tokens), lengths, item_table, in_weight, out_weight, grad_out)
            ]
        )
        return pl.pallas_call(
            deliver,
            name="deliver",
            out_shape=(
                jax.ShapeDtypeStruct((tokens, features), BF16),
                jax.ShapeDtypeStruct((shard_rows, features), F32),
            ),
            in_specs=[vmem, vmem],
            out_specs=(any_spec, any_spec),
            scratch_shapes=[pltpu.VMEM((shard_rows, features), F32), dma((DELIVERIES + 1,))],
            compiler_params=pltpu.CompilerParams(vmem_limit_bytes=8 * 1024 * 1024),
        )(mixed, table_grad.reshape(shard_rows, features))

    return jax.shard_map(
        shards,
        mesh=mesh,
        in_specs=(
            P(("dp", "rows")),
            P(("dp", "rows"), None),
            P("rows", None),
            P(),
            P(),
            P(("dp", "rows"), None),
        ),
        out_specs=(P(("dp", "rows"), None), P("rows", None)),
        check_vma=False,
    )
```
